32 devices in a mesh: gx: 4 (over y, core), gy: 8 (over z, x).
Axes of the slice: x: 2, y: 2, z: 4, core: 2. Of those that a mesh axis runs over, the one named last changes fastest.
Arguments:
- radiation: float32 [2, 4, 8, 64, 1024], P(None, None, None, 'gx', 'gy'), may hold values from -4 to 4, as said below
- ion_fraction: float32 [8, 64, 1024], P(None, 'gx', 'gy'), may hold values from 0.05 to 0.95
- density: float32 [8, 64, 1024], P(None, 'gx', 'gy'), may hold values from 0.1 to 10
- star_lum: float32 [4, 8, 2, 256], P('gx', 'gy'), may hold values from 0.1 to 10
- star_cell: int32 [4, 8, 3, 256], P('gx', 'gy'), may hold values from 0 to 127, as said below
- star_offset: float32 [4, 8, 3, 256], P('gx', 'gy'), may hold values from 0 to 1
- star_count: int32 [4, 8], P('gx', 'gy'), may hold values from 1 to 256, as said below
Outputs:
- radiation_out: float32 [2, 4, 8, 64, 1024], P(None, None, None, 'gx', 'gy')
- ion_out: float32 [8, 64, 1024], P(None, 'gx', 'gy')
The draws below stay inside these ranges and needn't reach their ends.
Inputs may be any that keep to these rules, and one draw needn't show every extreme that they name: `star_cell`: per slot: row 0 is the x corner within the tile, 0 to 15; row 1 the y corner, 0 to 127; row 2 the z corner, 0 to 7. `star_count`: some tile has all 256 slots live in every draw. `radiation`: N is positive and |F| < N in every cell.
All inputs are finite; a program needn't handle non-finite values.
Results may differ from the reference program's by a relative error of at most 0.0001.
Values sent between devices are 32-bit elements; how exact they have to be, the bound alone decides.
No kernel may reach another device: no remote copies, remote signals or barrier semaphores. Data moves between devices by JAX's collectives and lax.ppermute only.
A program may use at most 64 MiB of HBM per device.

```python
import math
import jax
import jax.numpy as jnp
from jax import lax

G = 2
CX = 16
CY = 128
NZ = 8
S_DEV = 256
SUBSTEPS = 4
CHEM_ITERS = 3
NX = 64
NY = 1024
TILES_X = 4
TILES_Y = 8


def draw_radiation(key, part):
    key_n = jax.random.fold_in(key, 11)
    key_d = jax.random.fold_in(key, 12)
    key_r = jax.random.fold_in(key, 13)
    shape = (G, NZ, NX, NY)
    low, high, reach = (0.1, 2.0, 0.9)
    photons = jnp.exp(jax.random.uniform(key_n, shape, jnp.float32, jnp.log(low), jnp.log(high)))
    direction = jax.random.normal(key_d, (G, 3, NZ, NX, NY), jnp.float32)
    length = jnp.sqrt(jnp.sum(direction * direction, axis=1, keepdims=True)) + 1e-06
    ratio = jax.random.uniform(key_r, shape, jnp.float32, 0.0, reach)
    flux = direction / length * (photons * ratio)[:, None]
    return jnp.concatenate([photons[:, None], flux], axis=1)


def draw_star_cell(key, part):
    shape = (TILES_X, TILES_Y, S_DEV)
    xs = jax.random.randint(jax.random.fold_in(key, 21), shape, 0, CX)
    ys = jax.random.randint(jax.random.fold_in(key, 22), shape, 0, CY)
    zs = jax.random.randint(jax.random.fold_in(key, 23), shape, 0, NZ)
    return jnp.stack([xs, ys, zs], axis=2).astype(jnp.int32)


def draw_star_count(key, part):
    divisor = jax.random.randint(jax.random.fold_in(key, 31), (TILES_X * TILES_Y,), 1, 9)
    counts = S_DEV // divisor
    chosen = jax.random.randint(jax.random.fold_in(key, 32), (), 0, TILES_X * TILES_Y)
    counts = counts.at[chosen].set(S_DEV)
    return counts.reshape(TILES_X, TILES_Y).astype(jnp.int32)


def block_scale(key, shape, shards, low, top_value):
    level, own = 1.0, jax.random.fold_in(key, 6)
    for axis_at, blocks in shards:
        steps = jnp.exp(jax.random.uniform(jax.random.fold_in(own, axis_at), (blocks,), jnp.float32, low / len(shards), top_value / len(shards)))
        level = level * jnp.repeat(steps, shape[axis_at] // blocks).reshape([-1 if axis == axis_at else 1 for axis in range(len(shape))])
    return level


def setup_inputs(seed: int = 0) -> dict:
    seeds = jax.random.split(jax.random.key(seed), 8)
    return {
        "radiation": draw_radiation(jax.random.fold_in(seeds[7], 71), 0),
        "ion_fraction": jnp.clip(0.05 + 0.9 * jax.random.uniform(seeds[1], (NZ, NX, NY), jnp.float32) ** block_scale(seeds[1], (NZ, NX, NY), ((1, 4), (2, 8)), -0.2, 0.2), 0.05, 0.95),
        "density": jnp.clip(jnp.exp(math.log(10.0) - 4.6051702 * jax.random.uniform(seeds[2], (NZ, NX, NY), jnp.float32) ** block_scale(seeds[2], (NZ, NX, NY), ((1, 4), (2, 8)), -0.2, 0.2)), 0.1, 10.0),
        "star_lum": jnp.clip(jnp.exp(math.log(10.0) - 4.6051702 * jax.random.uniform(seeds[3], (TILES_X, TILES_Y, G, S_DEV), jnp.float32) ** block_scale(seeds[3], (TILES_X, TILES_Y, G, S_DEV), ((0, 4), (1, 8)), -0.2, 0.2)), 0.1, 10.0),
        "star_cell": draw_star_cell(jax.random.fold_in(seeds[7], 71), 0),
        "star_offset": jnp.clip(1.0 * jax.random.uniform(seeds[5], (TILES_X, TILES_Y, 3, S_DEV), jnp.float32) ** block_scale(seeds[5], (TILES_X, TILES_Y, 3, S_DEV), ((0, 4), (1, 8)), -0.2, 0.2), 0.0, 1.0),
        "star_count": draw_star_count(jax.random.fold_in(seeds[7], 71), 0),
    }


DT = 0.3
ALPHA = 0.4
SIGMA = (1.5, 0.5)

def directional(state, axis_dir):
    photons = state[:, 0]
    flux = state[:, 1:4]
    fsq = jnp.minimum(lax.optimization_barrier(jnp.sum(flux * flux, axis=1)) / (photons * photons), 1.0)
    root = jnp.sqrt(4.0 - 3.0 * fsq)
    chi = (3.0 + 4.0 * fsq) / (5.0 + 2.0 * root)
    shape_term = (3.0 / (2.0 + root) + 6.0) / (5.0 + 2.0 * root)
    diag = 0.5 * (1.0 - chi) * photons
    scaled = shape_term / photons
    comps = [flux[:, axis_dir]]
    for other in range(3):
        value = scaled * flux[:, axis_dir] * flux[:, other]
        if other == axis_dir:
            value = value + diag
        comps.append(value)
    return jnp.stack(comps, axis=1)

def transport(state):
    total = jnp.zeros_like(state)
    for axis_dir, axis in ((0, 3), (1, 4), (2, 2)):
        phys = directional(state, axis_dir)
        face = 0.5 * (phys + jnp.roll(phys, -1, axis)) - 0.5 * (jnp.roll(state, -1, axis) - state)
        total = total + face - jnp.roll(face, 1, axis)
    return state - DT * total

def chemistry(state, ion, dens):
    sig = jnp.array(SIGMA, jnp.float32).reshape(2, 1, 1, 1)
    start_n = state[:, 0]
    start_f = state[:, 1:4]
    frac = ion
    for step in range(CHEM_ITERS):
        atten = 1.0 / (1.0 + DT * sig * dens * (1.0 - frac))
        photons = start_n * atten
        gamma = lax.optimization_barrier(jnp.sum(sig * photons, axis=0))
        frac = (ion + DT * gamma) / (1.0 + DT * (gamma + ALPHA * dens * frac))
    return (jnp.concatenate([photons[:, None], start_f * atten[:, None]], axis=1), frac)

def deposit(star_lum, star_cell, star_offset, star_count):
    slots = jnp.arange(S_DEV, dtype=jnp.int32)
    live = (slots[None, None, :] < star_count[:, :, None]).astype(jnp.float32)
    tile_x = jnp.arange(TILES_X, dtype=jnp.int32)[:, None, None]
    tile_y = jnp.arange(TILES_Y, dtype=jnp.int32)[None, :, None]
    cell_x = star_cell[:, :, 0] + tile_x * CX
    cell_y = star_cell[:, :, 1] + tile_y * CY
    cell_z = star_cell[:, :, 2]
    emission = jnp.zeros((G, NZ * NX * NY), jnp.float32)
    for dz in (0, 1):
        for dx in (0, 1):
            for dy in (0, 1):
                wz = star_offset[:, :, 2] if dz else 1.0 - star_offset[:, :, 2]
                wx = star_offset[:, :, 0] if dx else 1.0 - star_offset[:, :, 0]
                wy = star_offset[:, :, 1] if dy else 1.0 - star_offset[:, :, 1]
                weight = wz * wx * wy * live
                index = ((cell_z + dz) % NZ * NX + (cell_x + dx) % NX) * NY + (cell_y + dy) % NY
                values = jnp.moveaxis(star_lum * weight[:, :, None, :], 2, 0).reshape(G, -1)
                emission = emission.at[:, index.reshape(-1)].add(values)
    return emission.reshape(G, NZ, NX, NY)

def reference(radiation, ion_fraction, density, star_lum, star_cell, star_offset, star_count):
    emission = deposit(star_lum, star_cell, star_offset, star_count)
    state = radiation
    ion = ion_fraction
    for step in range(SUBSTEPS):
        state = transport(state)
        state = jnp.concatenate([state[:, :1] + DT * emission[:, None], state[:, 1:]], axis=1)
        state, ion = chemistry(state, ion, density)
    return (state, ion)
```

```python
import jax
import jax.numpy as jnp
from jax import lax
from jax.experimental import pallas as pl
from jax.experimental.pallas import tpu as pltpu
from jax.sharding import PartitionSpec as P

SUBSTEPS = 4
CHEM_ITERS = 3
DT = 0.3
ALPHA = 0.4
SIGMA = (1.5, 0.5)

HALO = SUBSTEPS
INNER = HALO - 1


def neighbour_pairs(count, parity):
    return [(i, (i + 1) % count if i % 2 == parity else (i - 1) % count) for i in range(count)]


def halo_rows(fields_full, fields_inner, depth):
    full = fields_full * HALO * depth
    return full, full + fields_inner * INNER * depth


def star_table(lum_ref, cell_ref, off_ref, count_ref):
    slots = lum_ref.shape[3]
    slot = lax.broadcasted_iota(jnp.int32, (1, slots), 1)
    live = (slot < count_ref[0, 0]).astype(jnp.float32)
    lum = [lum_ref[0, 0, g : g + 1, :] * live for g in range(lum_ref.shape[2])]
    cell = [cell_ref[0, 0, a : a + 1, :].astype(jnp.float32) for a in range(3)]
    off = [off_ref[0, 0, a : a + 1, :] for a in range(3)]
    return lum, cell, off


def deposit(stars, rows, depth, width):
    lum, cell, off = stars
    slots = lum[0].shape[1]
    z = lax.broadcasted_iota(jnp.int32, (depth, slots), 0).astype(jnp.float32)
    upper = cell[2] + 1.0
    upper = jnp.where(upper == float(depth), 0.0, upper)
    weight_z = jnp.where(z == cell[2], 1.0 - off[2], 0.0) + jnp.where(z == upper, off[2], 0.0)
    y = lax.broadcasted_iota(jnp.int32, (2 * width, slots), 0).astype(jnp.float32)
    weight_y = jnp.where(y == cell[1], 1.0 - off[1], 0.0) + jnp.where(y == cell[1] + 1.0, off[1], 0.0)
    left = []
    for light in lum:
        for x in rows:
            weight_x = jnp.where(cell[0] == float(x), 1.0 - off[0], 0.0)
            weight_x = weight_x + jnp.where(cell[0] == float(x - 1), off[0], 0.0)
            left.append(weight_z * (weight_x * light))
    return lax.dot_general(
        jnp.concatenate(left, axis=0),
        weight_y,
        (((1,), (1,)), ((), ())),
        precision=lax.Precision.HIGHEST,
        preferred_element_type=jnp.float32,
    )


def strip_lane():
    return lax.broadcasted_iota(jnp.int32, (8, 128), 1)


def to_strip(plane, group, lane, base):
    low = pltpu.roll(plane, (16 * group + 4) % 128, 1)
    high = pltpu.roll(plane, (16 * group + 12) % 128, 1)
    base = jnp.where((lane >= 16 * group) & (lane < 16 * group + 8), low, base)
    return jnp.where((lane >= 16 * group + 8) & (lane < 16 * group + 16), high, base)


def pack_kernel(rad, ion, den, lum_ref, cell_ref, off_ref, count_ref, out0, out1):
    even = lax.rem(lax.axis_index("gx"), 2) == 0
    groups, comps, depth, rows_x, width = rad.shape
    at = 0

    def put(high, low):
        nonlocal at
        out0[pl.ds(at, depth), :] = jnp.where(even, high, low)
        out1[pl.ds(at, depth), :] = jnp.where(even, low, high)
        at += depth

    for g in range(groups):
        for c in range(comps):
            for i in range(HALO):
                put(rad[g, c, :, rows_x - HALO + i, :], rad[g, c, :, i, :])
    for ref in (ion, den):
        for i in range(INNER):
            put(ref[:, rows_x - INNER + i, :], ref[:, i, :])
    lum, cell, off = star_table(lum_ref, cell_ref, off_ref, count_ref)
    table = jnp.concatenate(lum + cell + off, axis=0)
    for part in range(table.shape[1] // width):
        piece = table[:, part * width : (part + 1) * width]
        put(piece, piece)


def own_kernel(rad, ion, den, lum_ref, cell_ref, off_ref, count_ref, emis, strips):
    groups, comps, depth, rows_x, width = rad.shape
    stars = star_table(lum_ref, cell_ref, off_ref, count_ref)
    emis[...] = deposit(stars, range(rows_x + 1), depth, width)
    lane = strip_lane()
    fields = [(lambda x, g=g, c=c: rad[g, c, :, x, :]) for g in range(groups) for c in range(comps)]
    fields += [lambda x: ion[:, x, :], lambda x: den[:, x, :]]
    for f, read in enumerate(fields):
        for v in range(rows_x // 8):
            acc = jnp.zeros((8, 128), jnp.float32)
            for group in range(8):
                acc = to_strip(read(8 * v + group), group, lane, acc)
            strips[f, v] = acc


def edge_kernel(from0, from1, emis, strips_own, sent, own_e, centre_e):
    even = lax.rem(lax.axis_index("gx"), 2) == 0
    fields, owned, depth, width = strips_own.shape
    groups = own_e.shape[0]
    rows_x = 8 * owned
    lane = strip_lane()
    full, inner = halo_rows(fields - 2, 2, depth)

    def beside(at, size=None):
        size = depth if size is None else size
        first, second = from0[pl.ds(at, size), :], from1[pl.ds(at, size), :]
        return jnp.where(even, second, first), jnp.where(even, first, second)

    for f in range(fields):
        acc = jnp.zeros((8, 128), jnp.float32)
        for i in range(HALO):
            if f < fields - 2:
                below, above = beside((f * HALO + i) * depth)
                low_at, high_at = i, i + HALO
            elif i < INNER:
                below, above = beside(full + ((f - fields + 2) * INNER + i) * depth)
                low_at, high_at = i, i + HALO + 1
            else:
                continue
            acc = to_strip(above, low_at, lane, acc)
            acc = to_strip(below, high_at, lane, acc)
        for v in range(owned):
            sent[f, v] = strips_own[f, v]
        sent[f, owned] = acc

    parts = [beside(inner + p * depth) for p in range((from0.shape[0] - inner) // depth)]

    def stars_of(side):
        table = jnp.concatenate([part[side] for part in parts], axis=1)
        row = [table[k : k + 1, :] for k in range(table.shape[0])]
        return row[:groups], row[groups : groups + 3], row[groups + 3 : groups + 6]

    low_rows = list(range(rows_x - INNER, rows_x + 1))
    high_rows = list(range(INNER))
    below_e = deposit(stars_of(0), low_rows, depth, width)
    above_e = deposit(stars_of(1), high_rows, depth, width)

    def row_of(table, count, g, index, half):
        start = (g * count + index) * depth
        return table[start : start + depth, half * width : (half + 1) * width]

    def emission(g, x, half):
        parts = []
        if 0 <= x <= rows_x:
            start = (g * (rows_x + 1) + x) * depth
            parts.append(emis[start : start + depth, half * width : (half + 1) * width])
        if x <= 0:
            parts.append(row_of(below_e, len(low_rows), g, x + INNER, half))
        if x >= rows_x:
            parts.append(row_of(above_e, len(high_rows), g, x - rows_x, half))
        return sum(parts[1:], parts[0])

    for g in range(groups):
        acc_sent = [jnp.zeros((8, 128), jnp.float32)] * (owned + 1)
        acc_own = [jnp.zeros((8, 128), jnp.float32)] * (owned + 1)
        for x in range(-INNER, rows_x + INNER):
            row = x % (rows_x + 8)
            v, group = row // 8, row % 8
            plane, past = emission(g, x, 0), emission(g, x, 1)
            centre_e[g, x + HALO] = plane
            low = pltpu.roll(plane, (16 * group + 4) % 128, 1)
            high = pltpu.roll(plane, (16 * group + 12) % 128, 1)
            past_low = pltpu.roll(past, (16 * group + 4) % 128, 1)
            past_high = pltpu.roll(past, (16 * group + 12) % 128, 1)
            column = lane - 16 * group
            s = jnp.where((column >= 4) & (column < 8), low, acc_sent[v])
            s = jnp.where((column >= 8) & (column < 12), high, s)
            acc_sent[v] = jnp.where(column == 12, past_high, s)
            o = jnp.where((column >= 0) & (column < 4), low, acc_own[v])
            o = jnp.where((column >= 12) & (column < 16), high, o)
            acc_own[v] = jnp.where(column == 4, past_low, o)
        for v in range(owned + 1):
            sent[fields + g, v] = acc_sent[v]
            own_e[g, v] = acc_own[v]


def closure(state):
    photons, flux = state[0], state[1:]
    inverse = 1.0 / photons
    unit = [f * inverse for f in flux]
    fsq = jnp.minimum(unit[0] * unit[0] + unit[1] * unit[1] + unit[2] * unit[2], 1.0)
    square = 4.0 - 3.0 * fsq
    root = square * lax.rsqrt(square)
    shape_term = 3.0 / (2.0 + root)
    diag = (root - 1.0) * (photons * (1.0 / 3.0))
    scaled = [f * shape_term for f in flux]
    xx, yy, zz = (scaled[a] * unit[a] + diag for a in range(3))
    xy, xz, yz = scaled[0] * unit[1], scaled[0] * unit[2], scaled[1] * unit[2]
    return ((flux[0], xx, xy, xz), (flux[1], xy, yy, yz), (flux[2], xz, yz, zz))


def chemistry(state, ion, dens):
    groups = len(state)
    reach = DT * dens
    loss = ALPHA * reach
    push = [state[g][0] * (DT * SIGMA[g]) for g in range(groups)]
    frac = ion
    for step in range(CHEM_ITERS):
        free = reach * (1.0 - frac)
        atten = [1.0 / (1.0 + SIGMA[g] * free) for g in range(groups)]
        gamma = sum((push[g] * atten[g] for g in range(1, groups)), push[0] * atten[0])
        frac = (ion + gamma) / (1.0 + (gamma + loss * frac))
    return [[u * atten[g] for u in state[g]] for g in range(groups)], frac


def step_kernel(
    rad, ion, den, from0, from1, sent_own, own_e, from_low, from_high, centre_e,
    rad_out, ion_out, u_ref, ion_ref, den_ref, s_ref, e_ref, t_ref,
):
    even = lax.rem(lax.axis_index("gx"), 2) == 0
    groups, comps, depth, rows_x, width = rad.shape
    tiles = sent_own.shape[1]
    cycle = 8 * tiles
    fields = groups * comps
    full, _ = halo_rows(fields, 2, depth)
    lane = strip_lane()
    column = lax.rem(lane, 16)

    def beside(at):
        first, second = from0[pl.ds(at, depth), :], from1[pl.ds(at, depth), :]
        return jnp.where(even, second, first), jnp.where(even, first, second)

    for g in range(groups):
        for c in range(comps):
            f = g * comps + c
            for x in range(rows_x):
                u_ref[f, x + HALO] = rad[g, c, :, x, :]
            for i in range(HALO):
                below, above = beside((f * HALO + i) * depth)
                u_ref[f, i] = below
                u_ref[f, rows_x + HALO + i] = above
    for k, (src, dst) in enumerate(((ion, ion_ref), (den, den_ref))):
        for x in range(rows_x):
            dst[x + HALO] = src[:, x, :]
        for i in range(INNER):
            below, above = beside(full + (k * INNER + i) * depth)
            dst[i + 1] = below
            dst[rows_x + HALO + i] = above

    from_right = (column >= 4) & (column < 8)
    from_left = (column >= 8) & (column < 12)
    for f in range(fields + 2):
        for v in range(tiles):
            s_ref[f, v] = jnp.where(
                from_right, from_high[f, v], jnp.where(from_left, from_low[f, v], sent_own[f, v])
            )
    for g in range(groups):
        for v in range(tiles):
            f = fields + 2 + g
            e = own_e[g, v] + jnp.where(from_right, from_high[f, v], 0.0)
            e = e + jnp.where((column >= 8) & (column < 13), from_low[f, v], 0.0)
            s_ref[f, v] = e * DT
        for x in range(-INNER, rows_x + INNER):
            row = x % cycle
            v, group = row // 8, row % 8
            edge = pltpu.roll(s_ref[fields + 2 + g, v], (116 - 16 * group) % 128, 1)
            e_ref[g, x + HALO] = jnp.where(lane == 0, edge, centre_e[g, x + HALO] * DT)

    keep, share = 1.0 - 3.0 * DT, 0.5 * DT
    for step in range(SUBSTEPS):
        states = [
            [[s_ref[g * comps + c, v] for c in range(comps)] for g in range(groups)]
            for v in range(tiles)
        ]
        phys = [[closure(states[v][g]) for g in range(groups)] for v in range(tiles)]
        for v in range(tiles):
            for g in range(groups):
                for c in range(comps):
                    u, f = states[v][g][c], phys[v][g][1][c]
                    t_ref[g * comps + c, v] = jnp.where(
                        column == 11, u + f, pltpu.roll(u - f, 6, 1)
                    )
        if step < SUBSTEPS - 1:
            for v in range(tiles):
                new = []
                for g in range(groups):
                    comp = []
                    for c in range(comps):
                        u = states[v][g][c]
                        fx, fy, fz = (phys[v][g][a][c] for a in range(3))
                        vn, vp = (v + 1) % tiles, (v - 1) % tiles
                        down, here_d = states[vn][g][c] - phys[vn][g][0][c], u - fx
                        up, here_u = states[vp][g][c] + phys[vp][g][0][c], u + fx
                        total = jnp.where(
                            lane < 112, pltpu.roll(here_d, 112, 1), pltpu.roll(down, 112, 1)
                        )
                        total = total + jnp.where(
                            lane < 16, pltpu.roll(up, 16, 1), pltpu.roll(here_u, 16, 1)
                        )
                        total = total + pltpu.roll(u - fy, 127, 1) + pltpu.roll(u + fy, 1, 1)
                        total = total + pltpu.roll(u - fz, depth - 1, 0) + pltpu.roll(u + fz, 1, 0)
                        comp.append(keep * u + share * total)
                    comp[0] = comp[0] + s_ref[fields + 2 + g, v]
                    new.append(comp)
                new, frac = chemistry(new, s_ref[fields, v], s_ref[fields + 1, v])
                for g in range(groups):
                    for c in range(comps):
                        s_ref[g * comps + c, v] = new[g][c]
                s_ref[fields, v] = frac

        reach = SUBSTEPS - 1 - step

        def row_terms(x):
            row = x % cycle
            v, group = row // 8, row % 8
            up, down, rest = [], [], []
            for g in range(groups):
                state = [u_ref[g * comps + c, x + HALO] for c in range(comps)]
                px, py, pz = closure(state)
                for c in range(comps):
                    u = state[c]
                    up.append(u + px[c])
                    down.append(u - px[c])
                    if -reach <= x < rows_x + reach:
                        edge = pltpu.roll(t_ref[g * comps + c, v], (117 - 16 * group) % 128, 1)
                        total = jnp.where(lane == width - 1, edge, pltpu.roll(u - py[c], width - 1, 1))
                        total = total + jnp.where(lane == 0, edge, pltpu.roll(u + py[c], 1, 1))
                        total = total + pltpu.roll(u - pz[c], depth - 1, 0)
                        total = total + pltpu.roll(u + pz[c], 1, 0)
                        rest.append(keep * u + share * total)
            return up, down, rest

        before, _, _ = row_terms(-reach - 1)
        here, _, rest = row_terms(-reach)
        for x in range(-reach, rows_x + reach):
            after, down, rest_after = row_terms(x + 1)
            new = []
            for g in range(groups):
                comp = []
                for c in range(comps):
                    k = g * comps + c
                    comp.append(rest[k] + share * (before[k] + down[k]))
                comp[0] = comp[0] + e_ref[g, x + HALO]
                new.append(comp)
            new, frac = chemistry(new, ion_ref[x + HALO], den_ref[x + HALO])
            last = step == SUBSTEPS - 1
            for g in range(groups):
                for c in range(comps):
                    if last:
                        rad_out[g, c, :, x, :] = new[g][c]
                    else:
                        u_ref[g * comps + c, x + HALO] = new[g][c]
            if last:
                ion_out[:, x, :] = frac
            else:
                ion_ref[x + HALO] = frac
            before, here, rest = here, after, rest_after


def on_device(radiation, ion_fraction, density, star_lum, star_cell, star_offset, star_count):
    groups, comps, depth, rows_x, width = radiation.shape
    slots = star_lum.shape[3]
    if depth != 8 or width != 128 or rows_x % 8 or comps != 4 or slots % width:
        raise ValueError("tile shape")
    nx, ny = lax.axis_size("gx"), lax.axis_size("gy")
    if nx % 2:
        raise ValueError("odd axis")
    fields = groups * comps
    owned = rows_x // 8
    tiles = owned + 1
    _, inner = halo_rows(fields, 2, depth)
    halo = inner + (groups + 6) * (slots // width)
    f32 = jnp.float32
    vmem = pl.BlockSpec(memory_space=pltpu.VMEM)
    smem = pl.BlockSpec(memory_space=pltpu.SMEM)
    arrays = (radiation, ion_fraction, density, star_lum, star_cell, star_offset, star_count)
    arg_specs = [vmem] * 6 + [smem]

    to0, to1 = pl.pallas_call(
        pack_kernel,
        out_shape=[jax.ShapeDtypeStruct((halo, width), f32)] * 2,
        in_specs=arg_specs,
        name="pack_x",
    )(*arrays)
    from0 = lax.ppermute(to0, "gx", neighbour_pairs(nx, 0))
    from1 = lax.ppermute(to1, "gx", neighbour_pairs(nx, 1))
    emis, strips = pl.pallas_call(
        own_kernel,
        out_shape=[
            jax.ShapeDtypeStruct((groups * (rows_x + 1) * depth, 2 * width), f32),
            jax.ShapeDtypeStruct((fields + 2, owned, 8, width), f32),
        ],
        in_specs=arg_specs,
        cost_estimate=pl.CostEstimate(flops=30_000_000, bytes_accessed=1_000_000, transcendentals=0),
        name="own_edges",
    )(*arrays)
    sent, own_e, centre_e = pl.pallas_call(
        edge_kernel,
        out_shape=[
            jax.ShapeDtypeStruct((fields + 2 + groups, tiles, 8, width), f32),
            jax.ShapeDtypeStruct((groups, tiles, 8, width), f32),
            jax.ShapeDtypeStruct((groups, rows_x + 2 * HALO, depth, width), f32),
        ],
        in_specs=[vmem] * 4,
        name="edges",
    )(from0, from1, emis, strips)
    from_low = lax.ppermute(sent, "gy", [(i, (i + 1) % ny) for i in range(ny)])
    from_high = lax.ppermute(sent, "gy", [((i + 1) % ny, i) for i in range(ny)])
    plane = (depth, width)
    rows = rows_x + 2 * HALO
    return tuple(
        pl.pallas_call(
            step_kernel,
            out_shape=[
                jax.ShapeDtypeStruct(radiation.shape, f32),
                jax.ShapeDtypeStruct(ion_fraction.shape, f32),
            ],
            in_specs=[vmem] * 10,
            scratch_shapes=[
                pltpu.VMEM((fields, rows) + plane, f32),
                pltpu.VMEM((rows,) + plane, f32),
                pltpu.VMEM((rows,) + plane, f32),
                pltpu.VMEM((fields + 2 + groups, tiles) + plane, f32),
                pltpu.VMEM((groups, rows) + plane, f32),
                pltpu.VMEM((fields, tiles) + plane, f32),
            ],
            name="substeps",
        )(
            radiation, ion_fraction, density, from0, from1, sent, own_e, from_low, from_high, centre_e
        )
    )


def solution(mesh):
    return jax.shard_map(
        on_device,
        mesh=mesh,
        in_specs=(
            P(None, None, None, "gx", "gy"),
            P(None, "gx", "gy"),
            P(None, "gx", "gy"),
            P("gx", "gy", None, None),
            P("gx", "gy", None, None),
            P("gx", "gy", None, None),
            P("gx", "gy"),
        ),
        out_specs=(P(None, None, None, "gx", "gy"), P(None, "gx", "gy")),
        check_vma=False,
    )
```

```python
import jax
import jax.numpy as jnp
from jax import lax
from jax.experimental import pallas as pl
from jax.experimental.pallas import tpu as pltpu
from jax.sharding import PartitionSpec as P

SUBSTEPS = 4
CHEM_ITERS = 3
DT = 0.3
ALPHA = 0.4
SIGMA = (1.5, 0.5)

HALO = SUBSTEPS
INNER = HALO - 1


def neighbour_pairs(count, parity):
    return [(i, (i + 1) % count if i % 2 == parity else (i - 1) % count) for i in range(count)]


def halo_parts(fields_full, fields_inner, groups):
    inner = fields_full * HALO
    emis = inner + fields_inner * INNER
    return inner, emis, emis + groups * (INNER + 1)


def deposit(stars, rows, depth, width):
    lum, cell, off = stars
    slots = lum[0].shape[1]
    z = lax.broadcasted_iota(jnp.int32, (depth, slots), 0)
    upper = jnp.where(cell[2] + 1 == depth, 0, cell[2] + 1)
    weight_z = jnp.where(z == cell[2], 1.0 - off[2], 0.0) + jnp.where(z == upper, off[2], 0.0)
    y = lax.broadcasted_iota(jnp.int32, (2 * width, slots), 0)
    weight_y = jnp.where(y == cell[1], 1.0 - off[1], 0.0) + jnp.where(y == cell[1] + 1, off[1], 0.0)
    left = []
    for light in lum:
        for x in rows:
            weight_x = jnp.where(cell[0] == x, 1.0 - off[0], 0.0)
            weight_x = weight_x + jnp.where(cell[0] == x - 1, off[0], 0.0)
            left.append(weight_z * (weight_x * light))
    return lax.dot_general(
        jnp.concatenate(left, axis=0),
        weight_y,
        (((1,), (1,)), ((), ())),
        precision=lax.Precision.HIGHEST,
        preferred_element_type=jnp.float32,
    )


def strip_lane():
    return lax.broadcasted_iota(jnp.int32, (8, 128), 1)


def pack_kernel(
    rad_hbm, ion_hbm, den_hbm, lum_hbm, cell_hbm, off_hbm, count_ref,
    low_y, high_y, to0, to1, strips, emis,
    rad, ion, den, lum_ref, cell_ref, off_ref, sem,
):
    even = lax.rem(lax.axis_index("gx"), 2) == 0
    copies = [
        pltpu.make_async_copy(src, dst, sem.at[k])
        for k, (src, dst) in enumerate(
            (
                (lum_hbm, lum_ref),
                (cell_hbm, cell_ref),
                (off_hbm, off_ref),
                (rad_hbm, rad),
                (ion_hbm, ion),
                (den_hbm, den),
            )
        )
    ]
    for copy in copies:
        copy.start()
    groups, comps, depth, rows_x, width = rad.shape
    owned = rows_x // 8
    lane = strip_lane()
    column = lax.rem(lane, 16)
    zero = jnp.zeros((8, 128), jnp.float32)
    for copy in copies[:3]:
        copy.wait()
    slots = lum_ref.shape[3]
    slot = lax.broadcasted_iota(jnp.int32, (1, slots), 1)
    live = (slot < count_ref[0, 0]).astype(jnp.float32)
    stars = (
        [lum_ref[0, 0, g : g + 1, :] * live for g in range(groups)],
        [cell_ref[a] for a in range(3)],
        [off_ref[a] for a in range(3)],
    )
    table = deposit(stars, range(rows_x + 1), depth, width)

    def plane_of(g, x, half):
        start = (g * (rows_x + 1) + x) * depth
        return table[start : start + depth, half * width : (half + 1) * width]

    for copy in copies[3:]:
        copy.wait()
    reads = [(lambda x, g=g, c=c: rad[g, c, :, x, :]) for g in range(groups) for c in range(comps)]
    reads += [lambda x: ion[:, x, :], lambda x: den[:, x, :]]
    fields = len(reads)
    packs_low = [[zero] * owned for _ in range((fields + groups) // 4)]
    packs_high = [[zero] * owned for _ in range((fields + groups) // 4)]
    tail_low, tail_high = zero, zero

    def add(pack, k, part, source):
        return jnp.where((column >= 4 * k) & (column < 4 * k + 4), pltpu.roll(part, (4 * k - source) % 128, 1), pack)

    for f, read in enumerate(reads):
        for v in range(owned):
            acc = zero
            for group in range(8):
                plane = read(8 * v + group)
                low = pltpu.roll(plane, (16 * group + 4) % 128, 1)
                high = pltpu.roll(plane, (16 * group + 12) % 128, 1)
                at = lane - 16 * group
                acc = jnp.where((at >= 0) & (at < 8), low, jnp.where((at >= 8) & (at < 16), high, acc))
            strips[f, v] = acc
            p, k = f // 4, f % 4
            packs_high[p][v] = add(packs_high[p][v], k, acc, 8)
            packs_low[p][v] = add(packs_low[p][v], k, acc, 4)
    for g in range(groups):
        f = fields + g
        p, k = f // 4, f % 4
        sent, own = [zero] * (owned + 1), [zero] * (owned + 1)
        for x in range(rows_x + 1):
            v, group = x // 8, x % 8
            plane, past = plane_of(g, x, 0), plane_of(g, x, 1)
            emis[g, x] = plane
            low = pltpu.roll(plane, (16 * group + 4) % 128, 1)
            high = pltpu.roll(plane, (16 * group + 12) % 128, 1)
            past_low = pltpu.roll(past, (16 * group + 4) % 128, 1)
            past_high = pltpu.roll(past, (16 * group + 12) % 128, 1)
            at = lane - 16 * group
            s = jnp.where((at >= 4) & (at < 8), low, sent[v])
            s = jnp.where((at >= 8) & (at < 12), high, s)
            sent[v] = jnp.where(at == 12, past_high, s)
            o = jnp.where((at >= 0) & (at < 4), low, own[v])
            o = jnp.where((at >= 12) & (at < 16), high, o)
            own[v] = jnp.where(at == 4, past_low, o)
        for v in range(owned + 1):
            strips[f, v] = own[v]
        for v in range(owned):
            packs_high[p][v] = add(packs_high[p][v], k, sent[v], 9)
            packs_low[p][v] = add(packs_low[p][v], k, sent[v], 4)
        tail_high = add(tail_high, k, sent[owned], 9)
        tail_low = add(tail_low, k, sent[owned], 4)
    for p in range(len(packs_low)):
        for v in range(owned):
            high_y[p * owned + v] = packs_high[p][v]
            low_y[p * owned + v] = packs_low[p][v]
    high_y[len(packs_low) * owned] = tail_high
    low_y[len(packs_low) * owned] = tail_low

    at = 0

    def put(high, low):
        nonlocal at
        to0[at] = jnp.where(even, high, low)
        to1[at] = jnp.where(even, low, high)
        at += 1

    for g in range(groups):
        for c in range(comps):
            for i in range(HALO):
                put(rad[g, c, :, rows_x - HALO + i, :], rad[g, c, :, i, :])
    for ref in (ion, den):
        for i in range(INNER):
            put(ref[:, rows_x - INNER + i, :], ref[:, i, :])
    for g in range(groups):
        for i in range(INNER + 1):
            put(plane_of(g, rows_x - INNER + i, 0), plane_of(g, i, 0))


def edge_kernel(strips, from_low, from_high, joined, to0, to1):
    even = lax.rem(lax.axis_index("gx"), 2) == 0
    fields, tiles, depth, width = strips.shape
    owned = tiles - 1
    groups = len(SIGMA)
    lane = strip_lane()
    column = lax.rem(lane, 16)
    is_right = (column >= 4) & (column < 8)
    is_left = (column >= 8) & (column < 12)
    is_left_e = (column >= 9) & (column < 13)
    done = {}
    for f in range(fields):
        emission = f >= fields - groups
        p, k = f // 4, f % 4
        for v in range(tiles if emission else owned):
            at = p * owned + v
            right = pltpu.roll(from_high[at], (4 - 4 * k) % 128, 1)
            if emission:
                left = pltpu.roll(from_low[at], (9 - 4 * k) % 128, 1)
                value = strips[f, v] + jnp.where(is_right, right, 0.0) + jnp.where(is_left_e, left, 0.0)
            else:
                left = pltpu.roll(from_low[at], (8 - 4 * k) % 128, 1)
                value = jnp.where(is_right, right, jnp.where(is_left, left, strips[f, v]))
            joined[f, v] = value
            done[f, v] = value
    half = width // 2
    for p in range(fields // 2):
        a, b = 2 * p, 2 * p + 1
        high = jnp.where(lane >= half, done[a, owned - 1], pltpu.roll(done[b, owned - 1], half, 1))
        low = jnp.where(lane < half, done[a, 0], pltpu.roll(done[b, 0], half, 1))
        to0[p] = jnp.where(even, high, low)
        to1[p] = jnp.where(even, low, high)
    tail = jnp.zeros((8, 128), jnp.float32)
    for g in range(groups):
        moved = pltpu.roll(done[fields - groups + g, owned], 16 * g, 1) if g else done[fields - groups, owned]
        tail = jnp.where((lane >= 16 * g) & (lane < 16 * g + 16), moved, tail)
    to0[fields // 2] = tail
    to1[fields // 2] = tail


def closure(state):
    photons, flux = state[0], state[1:]
    inverse = 1.0 / photons
    unit = [f * inverse for f in flux]
    fsq = jnp.minimum(unit[0] * unit[0] + unit[1] * unit[1] + unit[2] * unit[2], 1.0)
    square = 4.0 - 3.0 * fsq
    root = square * lax.rsqrt(square)
    shape_term = 3.0 / (2.0 + root)
    diag = (root - 1.0) * (photons * (1.0 / 3.0))
    scaled = [f * shape_term for f in flux]
    xx, yy, zz = (scaled[a] * unit[a] + diag for a in range(3))
    xy, xz, yz = scaled[0] * unit[1], scaled[0] * unit[2], scaled[1] * unit[2]
    return ((flux[0], xx, xy, xz), (flux[1], xy, yy, yz), (flux[2], xz, yz, zz))


def chemistry(state, ion, dens):
    groups = len(state)
    reach = DT * dens
    loss = ALPHA * reach
    push = [state[g][0] * (DT * SIGMA[g]) for g in range(groups)]
    frac = ion
    for step in range(CHEM_ITERS):
        free = reach * (1.0 - frac)
        atten = [1.0 / (1.0 + SIGMA[g] * free) for g in range(groups)]
        gamma = sum((push[g] * atten[g] for g in range(1, groups)), push[0] * atten[0])
        frac = (ion + gamma) / (1.0 + (gamma + loss * frac))
    return [[u * atten[g] for u in state[g]] for g in range(groups)], frac


def step_kernel(
    rad, ion, den, from0, from1, joined, corner0, corner1, emis,
    rad_out, ion_out, u_ref, ion_ref, den_ref, s_ref, e_ref, t_ref,
):
    even = lax.rem(lax.axis_index("gx"), 2) == 0
    groups, comps, depth, rows_x, width = rad.shape
    tiles = joined.shape[1]
    owned = tiles - 1
    cycle = 8 * tiles
    fields = groups * comps
    inner_at, emis_at, _ = halo_parts(fields, 2, groups)
    lane = strip_lane()
    column = lax.rem(lane, 16)

    def beside(at, first=from0, second=from1):
        a, b = first[at], second[at]
        return jnp.where(even, b, a), jnp.where(even, a, b)

    for g in range(groups):
        for c in range(comps):
            f = g * comps + c
            for x in range(rows_x):
                u_ref[f, x + HALO] = rad[g, c, :, x, :]
            for i in range(HALO):
                below, above = beside(f * HALO + i)
                u_ref[f, i] = below
                u_ref[f, rows_x + HALO + i] = above
    for k, (src, dst) in enumerate(((ion, ion_ref), (den, den_ref))):
        for x in range(rows_x):
            dst[x + HALO] = src[:, x, :]
        for i in range(INNER):
            below, above = beside(inner_at + k * INNER + i)
            dst[i + 1] = below
            dst[rows_x + HALO + i] = above

    half = width // 2
    strip_fields = fields + 2 + groups
    for p in range(strip_fields // 2):
        below, above = beside(p, corner0, corner1)
        s_ref[2 * p, owned] = jnp.where(lane < half, above, below)
        s_ref[2 * p + 1, owned] = pltpu.roll(jnp.where(lane < half, below, above), half, 1)
        for f in (2 * p, 2 * p + 1):
            for v in range(owned):
                s_ref[f, v] = joined[f, v]
    tail, _ = beside(strip_fields // 2, corner0, corner1)
    for g in range(groups):
        f = fields + 2 + g
        row_16 = pltpu.roll(tail, (-16 * g) % 128, 1) if g else tail
        s_ref[f, 0] = (s_ref[f, 0] + jnp.where(lane < 16, row_16, 0.0)) * DT
        for v in range(1, owned):
            s_ref[f, v] = s_ref[f, v] * DT
        s_ref[f, owned] = (s_ref[f, owned] + joined[f, owned]) * DT
        for x in range(-INNER, rows_x + INNER):
            parts = []
            if 0 <= x <= rows_x:
                parts.append(emis[g, x])
            if x <= 0:
                parts.append(beside(emis_at + g * (INNER + 1) + x + INNER)[0])
            if x >= rows_x:
                parts.append(beside(emis_at + g * (INNER + 1) + x - rows_x)[1])
            total = sum(parts[1:], parts[0])
            row = x % cycle
            v, group = row // 8, row % 8
            edge = pltpu.roll(s_ref[f, v], (116 - 16 * group) % 128, 1)
            e_ref[g, x + HALO] = jnp.where(lane == 0, edge, total * DT)

    keep, share = 1.0 - 3.0 * DT, 0.5 * DT
    for step in range(SUBSTEPS):
        states = [
            [[s_ref[g * comps + c, v] for c in range(comps)] for g in range(groups)]
            for v in range(tiles)
        ]
        phys = [[closure(states[v][g]) for g in range(groups)] for v in range(tiles)]
        for v in range(tiles):
            for g in range(groups):
                for c in range(comps):
                    u, f = states[v][g][c], phys[v][g][1][c]
                    t_ref[g * comps + c, v] = jnp.where(
                        column == 11, u + f, pltpu.roll(u - f, 6, 1)
                    )
        if step < SUBSTEPS - 1:
            for v in range(tiles):
                new = []
                for g in range(groups):
                    comp = []
                    for c in range(comps):
                        u = states[v][g][c]
                        fx, fy, fz = (phys[v][g][a][c] for a in range(3))
                        vn, vp = (v + 1) % tiles, (v - 1) % tiles
                        down, here_d = states[vn][g][c] - phys[vn][g][0][c], u - fx
                        up, here_u = states[vp][g][c] + phys[vp][g][0][c], u + fx
                        total = jnp.where(
                            lane < 112, pltpu.roll(here_d, 112, 1), pltpu.roll(down, 112, 1)
                        )
                        total = total + jnp.where(
                            lane < 16, pltpu.roll(up, 16, 1), pltpu.roll(here_u, 16, 1)
                        )
                        total = total + pltpu.roll(u - fy, 127, 1) + pltpu.roll(u + fy, 1, 1)
                        total = total + pltpu.roll(u - fz, depth - 1, 0) + pltpu.roll(u + fz, 1, 0)
                        comp.append(keep * u + share * total)
                    comp[0] = comp[0] + s_ref[fields + 2 + g, v]
                    new.append(comp)
                new, frac = chemistry(new, s_ref[fields, v], s_ref[fields + 1, v])
                for g in range(groups):
                    for c in range(comps):
                        s_ref[g * comps + c, v] = new[g][c]
                s_ref[fields, v] = frac

        reach = SUBSTEPS - 1 - step

        def row_terms(x):
            row = x % cycle
            v, group = row // 8, row % 8
            up, down, rest = [], [], []
            for g in range(groups):
                state = [u_ref[g * comps + c, x + HALO] for c in range(comps)]
                px, py, pz = closure(state)
                for c in range(comps):
                    u = state[c]
                    up.append(u + px[c])
                    down.append(u - px[c])
                    if -reach <= x < rows_x + reach:
                        edge = pltpu.roll(t_ref[g * comps + c, v], (117 - 16 * group) % 128, 1)
                        total = jnp.where(lane == width - 1, edge, pltpu.roll(u - py[c], width - 1, 1))
                        total = total + jnp.where(lane == 0, edge, pltpu.roll(u + py[c], 1, 1))
                        total = total + pltpu.roll(u - pz[c], depth - 1, 0)
                        total = total + pltpu.roll(u + pz[c], 1, 0)
                        rest.append(keep * u + share * total)
            return up, down, rest

        before, _, _ = row_terms(-reach - 1)
        here, _, rest = row_terms(-reach)
        for x in range(-reach, rows_x + reach):
            after, down, rest_after = row_terms(x + 1)
            new = []
            for g in range(groups):
                comp = []
                for c in range(comps):
                    k = g * comps + c
                    comp.append(rest[k] + share * (before[k] + down[k]))
                comp[0] = comp[0] + e_ref[g, x + HALO]
                new.append(comp)
            new, frac = chemistry(new, ion_ref[x + HALO], den_ref[x + HALO])
            last = step == SUBSTEPS - 1
            for g in range(groups):
                for c in range(comps):
                    if last:
                        rad_out[g, c, :, x, :] = new[g][c]
                    else:
                        u_ref[g * comps + c, x + HALO] = new[g][c]
            if last:
                ion_out[:, x, :] = frac
            else:
                ion_ref[x + HALO] = frac
            before, here, rest = here, after, rest_after


def on_device(radiation, ion_fraction, density, star_lum, star_cell, star_offset, star_count):
    groups, comps, depth, rows_x, width = radiation.shape
    slots = star_lum.shape[3]
    fields = groups * comps
    strip_fields = fields + 2 + groups
    nx, ny = lax.axis_size("gx"), lax.axis_size("gy")
    if depth != 8 or width != 128 or rows_x % 8 or groups != len(SIGMA) or strip_fields % 4:
        raise ValueError("tile shape")
    if nx % 2:
        raise ValueError("odd axis")
    owned = rows_x // 8
    tiles = owned + 1
    f32 = jnp.float32
    plane = (depth, width)
    rows = rows_x + 2 * HALO
    planes = halo_parts(fields, 2, groups)[2]
    vmem = pl.BlockSpec(memory_space=pltpu.VMEM)
    smem = pl.BlockSpec(memory_space=pltpu.SMEM)
    hbm = pl.BlockSpec(memory_space=pltpu.HBM)
    small = pltpu.CompilerParams(vmem_limit_bytes=8 * 1024 * 1024)

    def out(*shape):
        return jax.ShapeDtypeStruct(shape + plane, f32)

    star_cell = star_cell.reshape(3, 1, slots)
    star_offset = star_offset.reshape(3, 1, slots)
    arrays = (radiation, ion_fraction, density, star_lum, star_cell, star_offset)
    sent = strip_fields // 4 * owned + 1
    low_y, high_y, to0, to1, strips, emis = pl.pallas_call(
        pack_kernel,
        out_shape=[
            out(sent), out(sent), out(planes), out(planes), out(strip_fields, tiles), out(groups, rows_x + 1)
        ],
        in_specs=[hbm] * 6 + [smem],
        scratch_shapes=[pltpu.VMEM(a.shape, a.dtype) for a in arrays] + [pltpu.SemaphoreType.DMA((6,))],
        compiler_params=small,
        name="pack",
    )(*[pltpu.with_memory_space_constraint(a, pltpu.HBM) for a in arrays], star_count)
    up = [(i, (i + 1) % ny) for i in range(ny)]
    down = [((i + 1) % ny, i) for i in range(ny)]
    from_low = lax.ppermute(high_y, "gy", up)
    from_high = lax.ppermute(low_y, "gy", down)
    from0 = lax.ppermute(to0, "gx", neighbour_pairs(nx, 0))
    from1 = lax.ppermute(to1, "gx", neighbour_pairs(nx, 1))
    joined, edge0, edge1 = pl.pallas_call(
        edge_kernel,
        out_shape=[out(strip_fields, tiles), out(strip_fields // 2 + 1), out(strip_fields // 2 + 1)],
        in_specs=[vmem] * 3,
        compiler_params=small,
        name="edges",
    )(strips, from_low, from_high)
    corner0 = lax.ppermute(edge0, "gx", neighbour_pairs(nx, 0))
    corner1 = lax.ppermute(edge1, "gx", neighbour_pairs(nx, 1))
    return tuple(
        pl.pallas_call(
            step_kernel,
            out_shape=[
                jax.ShapeDtypeStruct(radiation.shape, f32),
                jax.ShapeDtypeStruct(ion_fraction.shape, f32),
            ],
            in_specs=[vmem] * 9,
            scratch_shapes=[
                pltpu.VMEM((fields, rows) + plane, f32),
                pltpu.VMEM((rows,) + plane, f32),
                pltpu.VMEM((rows,) + plane, f32),
                pltpu.VMEM((strip_fields, tiles) + plane, f32),
                pltpu.VMEM((groups, rows) + plane, f32),
                pltpu.VMEM((fields, tiles) + plane, f32),
            ],
            compiler_params=small,
            name="substeps",
        )(radiation, ion_fraction, density, from0, from1, joined, corner0, corner1, emis)
    )


def solution(mesh):
    return jax.shard_map(
        on_device,
        mesh=mesh,
        in_specs=(
            P(None, None, None, "gx", "gy"),
            P(None, "gx", "gy"),
            P(None, "gx", "gy"),
            P("gx", "gy", None, None),
            P("gx", "gy", None, None),
            P("gx", "gy", None, None),
            P("gx", "gy"),
        ),
        out_specs=(P(None, None, None, "gx", "gy"), P(None, "gx", "gy")),
        check_vma=False,
    )
```

```python
import jax
import jax.numpy as jnp
from jax import lax
from jax.experimental import pallas as pl
from jax.experimental.pallas import tpu as pltpu
from jax.sharding import PartitionSpec as P

SUBSTEPS = 4
CHEM_ITERS = 3
DT = 0.3
ALPHA = 0.4
SIGMA = (1.5, 0.5)

HALO = SUBSTEPS
INNER = HALO - 1


def neighbour_pairs(count, parity):
    return [(i, (i + 1) % count if i % 2 == parity else (i - 1) % count) for i in range(count)]


def halo_parts(fields_full, fields_inner, groups):
    inner = fields_full * HALO
    emis = inner + fields_inner * INNER
    return inner, emis, emis + groups * (INNER + 1)


def deposit(stars, rows, depth, width):
    lum, cell, off = stars
    slots = lum[0].shape[1]
    z = lax.broadcasted_iota(jnp.int32, (depth, slots), 0)
    upper = jnp.where(cell[2] + 1 == depth, 0, cell[2] + 1)
    weight_z = jnp.where(z == cell[2], 1.0 - off[2], 0.0) + jnp.where(z == upper, off[2], 0.0)
    y = lax.broadcasted_iota(jnp.int32, (2 * width, slots), 0)
    weight_y = jnp.where(y == cell[1], 1.0 - off[1], 0.0) + jnp.where(y == cell[1] + 1, off[1], 0.0)
    left = []
    for light in lum:
        for x in rows:
            weight_x = jnp.where(cell[0] == x, 1.0 - off[0], 0.0)
            weight_x = weight_x + jnp.where(cell[0] == x - 1, off[0], 0.0)
            left.append(weight_z * (weight_x * light))
    return lax.dot_general(
        jnp.concatenate(left, axis=0),
        weight_y,
        (((1,), (1,)), ((), ())),
        precision=lax.Precision.HIGHEST,
        preferred_element_type=jnp.float32,
    )


def strip_lane():
    return lax.broadcasted_iota(jnp.int32, (8, 128), 1)


def pack_kernel(
    rad_hbm, ion_hbm, den_hbm, lum_hbm, cell_hbm, off_hbm, count_hbm,
    low_y, high_y, to0, to1, strips, emis,
    rad, ion, den, lum_ref, cell_ref, off_ref, count_ref, sem,
):
    even = lax.rem(lax.axis_index("gx"), 2) == 0
    copies = [
        pltpu.make_async_copy(src, dst, sem.at[k])
        for k, (src, dst) in enumerate(
            (
                (lum_hbm, lum_ref),
                (cell_hbm, cell_ref),
                (off_hbm, off_ref),
                (count_hbm, count_ref),
                (rad_hbm, rad),
                (ion_hbm, ion),
                (den_hbm, den),
            )
        )
    ]
    for copy in copies:
        copy.start()
    groups, comps, depth, rows_x, width = rad.shape
    owned = rows_x // 8
    lane = strip_lane()
    column = lax.rem(lane, 16)
    zero = jnp.zeros((8, 128), jnp.float32)
    for copy in copies[:4]:
        copy.wait()
    slots = lum_ref.shape[3]
    slot = lax.broadcasted_iota(jnp.int32, (1, slots), 1)
    live = (slot < count_ref[...]).astype(jnp.float32)
    stars = (
        [lum_ref[0, 0, g : g + 1, :] * live for g in range(groups)],
        [cell_ref[a] for a in range(3)],
        [off_ref[a] for a in range(3)],
    )
    table = deposit(stars, range(rows_x + 1), depth, width)

    def plane_of(g, x, half):
        start = (g * (rows_x + 1) + x) * depth
        return table[start : start + depth, half * width : (half + 1) * width]

    for copy in copies[4:]:
        copy.wait()
    reads = [(lambda x, g=g, c=c: rad[g, c, :, x, :]) for g in range(groups) for c in range(comps)]
    reads += [lambda x: ion[:, x, :], lambda x: den[:, x, :]]
    fields = len(reads)
    packs_low = [[zero] * owned for _ in range((fields + groups) // 4)]
    packs_high = [[zero] * owned for _ in range((fields + groups) // 4)]
    tail_low, tail_high = zero, zero

    def add(pack, k, part, source):
        return jnp.where((column >= 4 * k) & (column < 4 * k + 4), pltpu.roll(part, (4 * k - source) % 128, 1), pack)

    for f, read in enumerate(reads):
        for v in range(owned):
            acc = zero
            for group in range(8):
                plane = read(8 * v + group)
                low = pltpu.roll(plane, (16 * group + 4) % 128, 1)
                high = pltpu.roll(plane, (16 * group + 12) % 128, 1)
                at = lane - 16 * group
                acc = jnp.where((at >= 0) & (at < 8), low, jnp.where((at >= 8) & (at < 16), high, acc))
            strips[f, v] = acc
            p, k = f // 4, f % 4
            packs_high[p][v] = add(packs_high[p][v], k, acc, 8)
            packs_low[p][v] = add(packs_low[p][v], k, acc, 4)
    for g in range(groups):
        f = fields + g
        p, k = f // 4, f % 4
        sent, own = [zero] * (owned + 1), [zero] * (owned + 1)
        for x in range(rows_x + 1):
            v, group = x // 8, x % 8
            plane, past = plane_of(g, x, 0), plane_of(g, x, 1)
            emis[g, x] = plane
            low = pltpu.roll(plane, (16 * group + 4) % 128, 1)
            high = pltpu.roll(plane, (16 * group + 12) % 128, 1)
            past_low = pltpu.roll(past, (16 * group + 4) % 128, 1)
            past_high = pltpu.roll(past, (16 * group + 12) % 128, 1)
            at = lane - 16 * group
            s = jnp.where((at >= 4) & (at < 8), low, sent[v])
            s = jnp.where((at >= 8) & (at < 12), high, s)
            sent[v] = jnp.where(at == 12, past_high, s)
            o = jnp.where((at >= 0) & (at < 4), low, own[v])
            o = jnp.where((at >= 12) & (at < 16), high, o)
            own[v] = jnp.where(at == 4, past_low, o)
        for v in range(owned + 1):
            strips[f, v] = own[v]
        for v in range(owned):
            packs_high[p][v] = add(packs_high[p][v], k, sent[v], 9)
            packs_low[p][v] = add(packs_low[p][v], k, sent[v], 4)
        tail_high = add(tail_high, k, sent[owned], 9)
        tail_low = add(tail_low, k, sent[owned], 4)
    for p in range(len(packs_low)):
        for v in range(owned):
            high_y[p * owned + v] = packs_high[p][v]
            low_y[p * owned + v] = packs_low[p][v]
    high_y[len(packs_low) * owned] = tail_high
    low_y[len(packs_low) * owned] = tail_low

    at = 0

    def put(high, low):
        nonlocal at
        to0[at] = jnp.where(even, high, low)
        to1[at] = jnp.where(even, low, high)
        at += 1

    for g in range(groups):
        for c in range(comps):
            for i in range(HALO):
                put(rad[g, c, :, rows_x - HALO + i, :], rad[g, c, :, i, :])
    for ref in (ion, den):
        for i in range(INNER):
            put(ref[:, rows_x - INNER + i, :], ref[:, i, :])
    for g in range(groups):
        for i in range(INNER + 1):
            put(plane_of(g, rows_x - INNER + i, 0), plane_of(g, i, 0))


def edge_kernel(strips, from_low, from_high, joined, to0, to1):
    even = lax.rem(lax.axis_index("gx"), 2) == 0
    fields, tiles, depth, width = strips.shape
    owned = tiles - 1
    groups = len(SIGMA)
    lane = strip_lane()
    column = lax.rem(lane, 16)
    is_right = (column >= 4) & (column < 8)
    is_left = (column >= 8) & (column < 12)
    is_left_e = (column >= 9) & (column < 13)
    done = {}
    for f in range(fields):
        emission = f >= fields - groups
        p, k = f // 4, f % 4
        for v in range(tiles if emission else owned):
            at = p * owned + v
            right = pltpu.roll(from_high[at], (4 - 4 * k) % 128, 1)
            if emission:
                left = pltpu.roll(from_low[at], (9 - 4 * k) % 128, 1)
                value = strips[f, v] + jnp.where(is_right, right, 0.0) + jnp.where(is_left_e, left, 0.0)
            else:
                left = pltpu.roll(from_low[at], (8 - 4 * k) % 128, 1)
                value = jnp.where(is_right, right, jnp.where(is_left, left, strips[f, v]))
            joined[f, v] = value
            done[f, v] = value
    half = width // 2
    for p in range(fields // 2):
        a, b = 2 * p, 2 * p + 1
        high = jnp.where(lane >= half, done[a, owned - 1], pltpu.roll(done[b, owned - 1], half, 1))
        low = jnp.where(lane < half, done[a, 0], pltpu.roll(done[b, 0], half, 1))
        to0[p] = jnp.where(even, high, low)
        to1[p] = jnp.where(even, low, high)
    tail = jnp.zeros((8, 128), jnp.float32)
    for g in range(groups):
        moved = pltpu.roll(done[fields - groups + g, owned], 16 * g, 1) if g else done[fields - groups, owned]
        tail = jnp.where((lane >= 16 * g) & (lane < 16 * g + 16), moved, tail)
    to0[fields // 2] = tail
    to1[fields // 2] = tail


def closure(state):
    photons, flux = state[0], state[1:]
    inverse = 1.0 / photons
    unit = [f * inverse for f in flux]
    fsq = jnp.minimum(unit[0] * unit[0] + unit[1] * unit[1] + unit[2] * unit[2], 1.0)
    square = 4.0 - 3.0 * fsq
    root = square * lax.rsqrt(square)
    shape_term = 3.0 / (2.0 + root)
    diag = (root - 1.0) * (photons * (1.0 / 3.0))
    scaled = [f * shape_term for f in flux]
    xx, yy, zz = (scaled[a] * unit[a] + diag for a in range(3))
    xy, xz, yz = scaled[0] * unit[1], scaled[0] * unit[2], scaled[1] * unit[2]
    return ((flux[0], xx, xy, xz), (flux[1], xy, yy, yz), (flux[2], xz, yz, zz))


def chemistry(state, ion, dens):
    groups = len(state)
    reach = DT * dens
    loss = ALPHA * reach
    push = [state[g][0] * (DT * SIGMA[g]) for g in range(groups)]
    frac = ion
    for step in range(CHEM_ITERS):
        free = reach * (1.0 - frac)
        atten = [1.0 / (1.0 + SIGMA[g] * free) for g in range(groups)]
        gamma = sum((push[g] * atten[g] for g in range(1, groups)), push[0] * atten[0])
        frac = (ion + gamma) / (1.0 + (gamma + loss * frac))
    return [[u * atten[g] for u in state[g]] for g in range(groups)], frac


def strip_step(s_ref, t_ref, tiles, groups, comps, depth, update):
    fields = groups * comps
    keep, share = 1.0 - 3.0 * DT, 0.5 * DT
    lane = strip_lane()
    column = lax.rem(lane, 16)
    states = [
        [[s_ref[g * comps + c, v] for c in range(comps)] for g in range(groups)] for v in range(tiles)
    ]
    phys = [[closure(states[v][g]) for g in range(groups)] for v in range(tiles)]
    for v in range(tiles):
        for g in range(groups):
            for c in range(comps):
                u, f = states[v][g][c], phys[v][g][1][c]
                t_ref[g * comps + c, v] = jnp.where(column == 11, u + f, pltpu.roll(u - f, 6, 1))
    if not update:
        return
    for v in range(tiles):
        new = []
        for g in range(groups):
            comp = []
            for c in range(comps):
                u = states[v][g][c]
                fx, fy, fz = (phys[v][g][a][c] for a in range(3))
                vn, vp = (v + 1) % tiles, (v - 1) % tiles
                down, here_d = states[vn][g][c] - phys[vn][g][0][c], u - fx
                up, here_u = states[vp][g][c] + phys[vp][g][0][c], u + fx
                total = pltpu.roll(jnp.where(lane < 16, down, here_d), 112, 1)
                total = total + pltpu.roll(jnp.where(lane >= 112, up, here_u), 16, 1)
                total = total + pltpu.roll(u - fy, 127, 1) + pltpu.roll(u + fy, 1, 1)
                total = total + pltpu.roll(u - fz, depth - 1, 0) + pltpu.roll(u + fz, 1, 0)
                comp.append(keep * u + share * total)
            comp[0] = comp[0] + s_ref[fields + 2 + g, v]
            new.append(comp)
        new, frac = chemistry(new, s_ref[fields, v], s_ref[fields + 1, v])
        for g in range(groups):
            for c in range(comps):
                s_ref[g * comps + c, v] = new[g][c]
        s_ref[fields, v] = frac


def sweep(lo, hi, read, source, ion_of, den_of, write, t_ref, groups, comps, first_up=None, last_down=None):
    keep, share = 1.0 - 3.0 * DT, 0.5 * DT
    lane = strip_lane()
    depth, width = lane.shape
    cycle = 8 * t_ref.shape[1]

    def row_terms(x, inside):
        row = x % cycle
        v, group = row // 8, row % 8
        up, down, rest = [], [], []
        for g in range(groups):
            state = [read(g * comps + c, x) for c in range(comps)]
            px, py, pz = closure(state)
            for c in range(comps):
                u = state[c]
                up.append(u + px[c])
                down.append(u - px[c])
                if inside:
                    edge = pltpu.roll(t_ref[g * comps + c, v], (117 - 16 * group) % 128, 1)
                    total = jnp.where(lane == width - 1, edge, pltpu.roll(u - py[c], width - 1, 1))
                    total = total + jnp.where(lane == 0, edge, pltpu.roll(u + py[c], 1, 1))
                    total = total + pltpu.roll(u - pz[c], depth - 1, 0)
                    total = total + pltpu.roll(u + pz[c], 1, 0)
                    rest.append(keep * u + share * total)
        return up, down, rest

    before = row_terms(lo - 1, False)[0] if first_up is None else first_up
    here, low_down, rest = row_terms(lo, True)
    for x in range(lo, hi):
        if x + 1 < hi:
            after, down, rest_after = row_terms(x + 1, True)
        else:
            after, rest_after = None, None
            down = row_terms(hi, False)[1] if last_down is None else last_down
        new = []
        for g in range(groups):
            comp = []
            for c in range(comps):
                k = g * comps + c
                comp.append(rest[k] + share * (before[k] + down[k]))
            comp[0] = comp[0] + source(g, x)
            new.append(comp)
        new, frac = chemistry(new, ion_of(x), den_of(x))
        write(x, [new[g][c] for g in range(groups) for c in range(comps)], frac)
        if x + 1 < hi:
            before, here, rest = here, after, rest_after
    return low_down, here


def inner_kernel(rad, ion, den, joined, emis, u_ref, ion_ref, saved, s_ref, e_ref, t_ref):
    groups, comps, depth, rows_x, width = rad.shape
    tiles = rows_x // 8
    fields = groups * comps
    lane = strip_lane()
    for g in range(groups):
        for c in range(comps):
            for x in range(rows_x):
                u_ref[g * comps + c, x] = rad[g, c, :, x, :]
    for x in range(rows_x):
        ion_ref[x] = ion[:, x, :]
    for f in range(fields + 2):
        for v in range(tiles):
            s_ref[f, v] = joined[f, v]
    for g in range(groups):
        f = fields + 2 + g
        for v in range(tiles):
            s_ref[f, v] = joined[f, v] * DT
        for x in range(1, rows_x - 1):
            v, group = x // 8, x % 8
            edge = pltpu.roll(s_ref[f, v], (116 - 16 * group) % 128, 1)
            e_ref[g, x] = jnp.where(lane == 0, edge, emis[g, x] * DT)

    def write(x, values, frac):
        for k, value in enumerate(values):
            u_ref[k, x] = value
        ion_ref[x] = frac

    for step in range(SUBSTEPS):
        strip_step(s_ref, t_ref, tiles, groups, comps, depth, step < SUBSTEPS - 1)
        down, up = sweep(
            step + 1,
            rows_x - 1 - step,
            lambda k, x: u_ref[k, x],
            lambda g, x: e_ref[g, x],
            lambda x: ion_ref[x],
            lambda x: den[:, x, :],
            write,
            t_ref,
            groups,
            comps,
        )
        for k in range(fields):
            saved[0, step, k] = down[k]
            saved[1, step, k] = up[k]


def outer_kernel(
    u_mid, ion_mid, saved, den, from0, from1, joined, corner0, corner1, emis,
    rad_out, ion_out, u_ref, ion_ref, s_ref, e_ref, t_ref,
):
    even = lax.rem(lax.axis_index("gx"), 2) == 0
    groups, comps, depth, rows_x, width = rad_out.shape
    tiles = joined.shape[1]
    owned = tiles - 1
    cycle = 8 * tiles
    fields = groups * comps
    inner_at, emis_at, _ = halo_parts(fields, 2, groups)
    lane = strip_lane()

    def beside(at, first=from0, second=from1):
        a, b = first[at], second[at]
        return jnp.where(even, b, a), jnp.where(even, a, b)

    half = width // 2
    strip_fields = fields + 2 + groups
    for p in range(strip_fields // 2):
        below, above = beside(p, corner0, corner1)
        s_ref[2 * p, owned] = jnp.where(lane < half, above, below)
        s_ref[2 * p + 1, owned] = pltpu.roll(jnp.where(lane < half, below, above), half, 1)
        for f in (2 * p, 2 * p + 1):
            for v in range(owned):
                s_ref[f, v] = joined[f, v]
    edge_rows = list(range(-INNER, HALO)) + list(range(rows_x - HALO, rows_x + INNER))
    tail, _ = beside(strip_fields // 2, corner0, corner1)
    for g in range(groups):
        f = fields + 2 + g
        row_16 = pltpu.roll(tail, (-16 * g) % 128, 1) if g else tail
        s_ref[f, 0] = (s_ref[f, 0] + jnp.where(lane < 16, row_16, 0.0)) * DT
        for v in range(1, owned):
            s_ref[f, v] = s_ref[f, v] * DT
        s_ref[f, owned] = (s_ref[f, owned] + joined[f, owned]) * DT
        for x in edge_rows:
            parts = []
            if 0 <= x <= rows_x:
                parts.append(emis[g, x])
            if x <= 0:
                parts.append(beside(emis_at + g * (INNER + 1) + x + INNER)[0])
            if x >= rows_x:
                parts.append(beside(emis_at + g * (INNER + 1) + x - rows_x)[1])
            total = sum(parts[1:], parts[0])
            row = x % cycle
            v, group = row // 8, row % 8
            edge = pltpu.roll(s_ref[f, v], (116 - 16 * group) % 128, 1)
            e_ref[g, x + HALO] = jnp.where(lane == 0, edge, total * DT)

    for f in range(fields):
        for i in range(HALO):
            below, above = beside(f * HALO + i)
            u_ref[f, i] = below
            u_ref[f, rows_x + HALO + i] = above
            u_ref[f, HALO + i] = u_mid[f, i]
            u_ref[f, rows_x + i] = u_mid[f, rows_x - HALO + i]
    for i in range(HALO):
        ion_ref[HALO + i] = ion_mid[i]
        ion_ref[rows_x + i] = ion_mid[rows_x - HALO + i]
    for i in range(INNER):
        below, above = beside(inner_at + i)
        ion_ref[i + 1] = below
        ion_ref[rows_x + HALO + i] = above

    def den_of(x):
        if x < 0:
            return beside(inner_at + INNER + x + INNER)[0]
        if x >= rows_x:
            return beside(inner_at + INNER + x - rows_x)[1]
        return den[:, x, :]

    def finish(x, values, frac):
        for k, value in enumerate(values):
            rad_out[k // comps, k % comps, :, x, :] = value
        ion_out[:, x, :] = frac

    def write(x, values, frac):
        for k, value in enumerate(values):
            u_ref[k, x + HALO] = value
        ion_ref[x + HALO] = frac

    for x in range(HALO, rows_x - HALO):
        finish(x, [u_mid[k, x] for k in range(fields)], ion_mid[x])

    for step in range(SUBSTEPS):
        strip_step(s_ref, t_ref, tiles, groups, comps, depth, step < SUBSTEPS - 1)
        last = step == SUBSTEPS - 1
        common = (
            lambda k, x: u_ref[k, x + HALO],
            lambda g, x: e_ref[g, x + HALO],
            lambda x: ion_ref[x + HALO],
            den_of,
            finish if last else write,
            t_ref,
            groups,
            comps,
        )
        rest = INNER - step
        sweep(-rest, step + 1, *common, last_down=[saved[0, step, k] for k in range(fields)])
        sweep(
            rows_x - 1 - step,
            rows_x + rest,
            *common,
            first_up=[saved[1, step, k] for k in range(fields)],
        )


def on_device(radiation, ion_fraction, density, star_lum, star_cell, star_offset, star_count):
    groups, comps, depth, rows_x, width = radiation.shape
    slots = star_lum.shape[3]
    fields = groups * comps
    strip_fields = fields + 2 + groups
    nx, ny = lax.axis_size("gx"), lax.axis_size("gy")
    if depth != 8 or width != 128 or rows_x % 8 or groups != len(SIGMA) or strip_fields % 4 or rows_x < 2 * HALO:
        raise ValueError("tile shape")
    if nx % 2:
        raise ValueError("odd axis")
    owned = rows_x // 8
    tiles = owned + 1
    f32 = jnp.float32
    plane = (depth, width)
    rows = rows_x + 2 * HALO
    planes = halo_parts(fields, 2, groups)[2]
    vmem = pl.BlockSpec(memory_space=pltpu.VMEM)
    hbm = pl.BlockSpec(memory_space=pltpu.HBM)
    small = pltpu.CompilerParams(vmem_limit_bytes=8 * 1024 * 1024)

    def out(*shape):
        return jax.ShapeDtypeStruct(shape + plane, f32)

    star_cell = star_cell.reshape(3, 1, slots)
    star_offset = star_offset.reshape(3, 1, slots)
    arrays = (radiation, ion_fraction, density, star_lum, star_cell, star_offset, star_count)
    sent = strip_fields // 4 * owned + 1
    low_y, high_y, to0, to1, strips, emis = pl.pallas_call(
        pack_kernel,
        out_shape=[
            out(sent), out(sent), out(planes), out(planes), out(strip_fields, tiles), out(groups, rows_x + 1)
        ],
        in_specs=[hbm] * 7,
        scratch_shapes=[pltpu.VMEM(a.shape, a.dtype) for a in arrays] + [pltpu.SemaphoreType.DMA((7,))],
        compiler_params=small,
        name="pack",
    )(*[pltpu.with_memory_space_constraint(a, pltpu.HBM) for a in arrays[:6]], star_count)
    up = [(i, (i + 1) % ny) for i in range(ny)]
    down = [((i + 1) % ny, i) for i in range(ny)]
    from_low = lax.ppermute(high_y, "gy", up)
    from_high = lax.ppermute(low_y, "gy", down)
    from0 = lax.ppermute(to0, "gx", neighbour_pairs(nx, 0))
    from1 = lax.ppermute(to1, "gx", neighbour_pairs(nx, 1))
    joined, edge0, edge1 = pl.pallas_call(
        edge_kernel,
        out_shape=[out(strip_fields, tiles), out(strip_fields // 2 + 1), out(strip_fields // 2 + 1)],
        in_specs=[vmem] * 3,
        compiler_params=small,
        name="edges",
    )(strips, from_low, from_high)
    corner0 = lax.ppermute(edge0, "gx", neighbour_pairs(nx, 0))
    corner1 = lax.ppermute(edge1, "gx", neighbour_pairs(nx, 1))
    u_mid, ion_mid, saved = pl.pallas_call(
        inner_kernel,
        out_shape=[out(fields, rows_x), out(rows_x), out(2, SUBSTEPS, fields)],
        in_specs=[vmem] * 5,
        scratch_shapes=[
            pltpu.VMEM((strip_fields, owned) + plane, f32),
            pltpu.VMEM((groups, rows_x) + plane, f32),
            pltpu.VMEM((fields, owned) + plane, f32),
        ],
        compiler_params=small,
        cost_estimate=pl.CostEstimate(flops=40_000_000, bytes_accessed=2_000_000, transcendentals=0),
        name="inner_rows",
    )(radiation, ion_fraction, density, joined, emis)
    return tuple(
        pl.pallas_call(
            outer_kernel,
            out_shape=[
                jax.ShapeDtypeStruct(radiation.shape, f32),
                jax.ShapeDtypeStruct(ion_fraction.shape, f32),
            ],
            in_specs=[vmem] * 10,
            scratch_shapes=[
                pltpu.VMEM((fields, rows) + plane, f32),
                pltpu.VMEM((rows,) + plane, f32),
                pltpu.VMEM((strip_fields, tiles) + plane, f32),
                pltpu.VMEM((groups, rows) + plane, f32),
                pltpu.VMEM((fields, tiles) + plane, f32),
            ],
            compiler_params=small,
            name="outer_rows",
        )(u_mid, ion_mid, saved, density, from0, from1, joined, corner0, corner1, emis)
    )


def solution(mesh):
    return jax.shard_map(
        on_device,
        mesh=mesh,
        in_specs=(
            P(None, None, None, "gx", "gy"),
            P(None, "gx", "gy"),
            P(None, "gx", "gy"),
            P("gx", "gy", None, None),
            P("gx", "gy", None, None),
            P("gx", "gy", None, None),
            P("gx", "gy"),
        ),
        out_specs=(P(None, None, None, "gx", "gy"), P(None, "gx", "gy")),
        check_vma=False,
    )
```

```python
import jax
import jax.numpy as jnp
from jax import lax
from jax.experimental import pallas as pl
from jax.experimental.pallas import tpu as pltpu
from jax.sharding import PartitionSpec as P

SUBSTEPS = 4
CHEM_ITERS = 3
DT = 0.3
ALPHA = 0.4
SIGMA = (1.5, 0.5)

HALO = SUBSTEPS
INNER = HALO - 1


def neighbour_pairs(count, parity):
    return [(i, (i + 1) % count if i % 2 == parity else (i - 1) % count) for i in range(count)]


def halo_parts(fields_full, fields_inner, groups):
    inner = fields_full * HALO
    emis = inner + fields_inner * INNER
    return inner, emis, emis + groups * (INNER + 1)


def deposit(stars, rows, depth, width):
    lum, cell, off = stars
    slots = lum[0].shape[1]
    z = lax.broadcasted_iota(jnp.int32, (depth, slots), 0)
    upper = jnp.where(cell[2] + 1 == depth, 0, cell[2] + 1)
    weight_z = jnp.where(z == cell[2], 1.0 - off[2], 0.0) + jnp.where(z == upper, off[2], 0.0)
    y = lax.broadcasted_iota(jnp.int32, (2 * width, slots), 0)
    weight_y = jnp.where(y == cell[1], 1.0 - off[1], 0.0) + jnp.where(y == cell[1] + 1, off[1], 0.0)
    left = []
    for light in lum:
        for x in rows:
            weight_x = jnp.where(cell[0] == x, 1.0 - off[0], 0.0)
            weight_x = weight_x + jnp.where(cell[0] == x - 1, off[0], 0.0)
            left.append(weight_z * (weight_x * light))
    return lax.dot_general(
        jnp.concatenate(left, axis=0),
        weight_y,
        (((1,), (1,)), ((), ())),
        precision=lax.Precision.HIGHEST,
        preferred_element_type=jnp.float32,
    )


def sizes_of(emis, fields):
    groups, rows, depth, width = emis.shape
    return groups, fields // groups, depth, rows - 1, width


def strip_lane():
    return lax.broadcasted_iota(jnp.int32, (8, 128), 1)


def pack_kernel(
    rad_hbm, ion_hbm, den_hbm, lum_hbm, cell_hbm, off_hbm, count_hbm,
    low_y, high_y, to0, to1, strips, emis,
    rad, ion, den, lum_ref, cell_ref, off_ref, count_ref, sem,
):
    even = lax.rem(lax.axis_index("gx"), 2) == 0
    copies = [
        pltpu.make_async_copy(src, dst, sem.at[k])
        for k, (src, dst) in enumerate(
            (
                (lum_hbm, lum_ref),
                (cell_hbm, cell_ref),
                (off_hbm, off_ref),
                (count_hbm, count_ref),
                (rad_hbm, rad),
                (ion_hbm, ion),
                (den_hbm, den),
            )
        )
    ]
    for copy in copies:
        copy.start()
    groups, comps, depth, rows_x, width = sizes_of(emis, rad.shape[0])
    owned = rows_x // 8
    lane = strip_lane()
    column = lax.rem(lane, 16)
    zero = jnp.zeros((8, 128), jnp.float32)
    for copy in copies[:4]:
        copy.wait()
    slots = lum_ref.shape[3]
    slot = lax.broadcasted_iota(jnp.int32, (1, slots), 1)
    live = (slot < count_ref[...]).astype(jnp.float32)
    stars = (
        [lum_ref[0, 0, g : g + 1, :] * live for g in range(groups)],
        [cell_ref[a] for a in range(3)],
        [off_ref[a] for a in range(3)],
    )
    table = deposit(stars, range(rows_x + 1), depth, width)

    def plane_of(g, x, half):
        start = (g * (rows_x + 1) + x) * depth
        return table[start : start + depth, half * width : (half + 1) * width]

    for copy in copies[4:]:
        copy.wait()
    reads = [(lambda x, f=f: rad[f, pl.ds(x, depth, stride=rows_x), :]) for f in range(groups * comps)]
    reads += [lambda x: ion[pl.ds(x, depth, stride=rows_x), :], lambda x: den[pl.ds(x, depth, stride=rows_x), :]]
    fields = len(reads)
    packs_low = [[zero] * owned for _ in range((fields + groups) // 4)]
    packs_high = [[zero] * owned for _ in range((fields + groups) // 4)]
    tail_low, tail_high = zero, zero

    def add(pack, k, part, source):
        return jnp.where((column >= 4 * k) & (column < 4 * k + 4), pltpu.roll(part, (4 * k - source) % 128, 1), pack)

    for f, read in enumerate(reads):
        for v in range(owned):
            acc = zero
            for group in range(8):
                low = pltpu.roll(read(8 * v + group), (16 * group + 4) % 128, 1)
                at = lane - 16 * group
                acc = jnp.where((at >= 0) & (at < 8), low, acc)
            acc = jnp.where(column < 8, acc, pltpu.roll(acc, 8, 1))
            strips[f, v] = acc
            p, k = f // 4, f % 4
            packs_high[p][v] = add(packs_high[p][v], k, acc, 8)
            packs_low[p][v] = add(packs_low[p][v], k, acc, 4)
    for g in range(groups):
        f = fields + g
        p, k = f // 4, f % 4
        near, past = [zero] * (owned + 1), [zero] * (owned + 1)
        for x in range(rows_x + 1):
            v, group = x // 8, x % 8
            plane = plane_of(g, x, 0)
            emis[g, x] = plane
            at = lane - 16 * group
            low = pltpu.roll(plane, (16 * group + 4) % 128, 1)
            near[v] = jnp.where((at >= 0) & (at < 8), low, near[v])
            over = plane_of(g, x, 1)
            over = pltpu.roll(over, 16 * group, 1) if group else over
            past[v] = jnp.where(at == 0, over, past[v])
        sent, own = [], []
        for v in range(owned + 1):
            far = pltpu.roll(near[v], 8, 1)
            s = jnp.where((column >= 4) & (column < 8), near[v], 0.0)
            s = jnp.where((column >= 8) & (column < 12), far, s)
            sent.append(jnp.where(column == 12, pltpu.roll(past[v], 12, 1), s))
            o = jnp.where(column < 4, near[v], jnp.where(column >= 12, far, 0.0))
            own.append(jnp.where(column == 4, pltpu.roll(past[v], 4, 1), o))
        for v in range(owned + 1):
            strips[f, v] = own[v]
        for v in range(owned):
            packs_high[p][v] = add(packs_high[p][v], k, sent[v], 9)
            packs_low[p][v] = add(packs_low[p][v], k, sent[v], 4)
        tail_high = add(tail_high, k, sent[owned], 9)
        tail_low = add(tail_low, k, sent[owned], 4)
    for p in range(len(packs_low)):
        for v in range(owned):
            high_y[p * owned + v] = packs_high[p][v]
            low_y[p * owned + v] = packs_low[p][v]
    high_y[len(packs_low) * owned] = tail_high
    low_y[len(packs_low) * owned] = tail_low

    at = 0

    def put(high, low):
        nonlocal at
        to0[at] = jnp.where(even, high, low)
        to1[at] = jnp.where(even, low, high)
        at += 1

    for read in reads[: groups * comps]:
        for i in range(HALO):
            put(read(rows_x - HALO + i), read(i))
    for read in reads[groups * comps :]:
        for i in range(INNER):
            put(read(rows_x - INNER + i), read(i))
    for g in range(groups):
        for i in range(INNER + 1):
            put(plane_of(g, rows_x - INNER + i, 0), plane_of(g, i, 0))


def edge_kernel(strips, from_low, from_high, joined, to0, to1):
    even = lax.rem(lax.axis_index("gx"), 2) == 0
    fields, tiles, depth, width = strips.shape
    owned = tiles - 1
    groups = len(SIGMA)
    lane = strip_lane()
    column = lax.rem(lane, 16)
    is_right = (column >= 4) & (column < 8)
    is_left = (column >= 8) & (column < 12)
    is_left_e = (column >= 9) & (column < 13)
    done = {}
    for f in range(fields):
        emission = f >= fields - groups
        p, k = f // 4, f % 4
        for v in range(tiles if emission else owned):
            at = p * owned + v
            right = pltpu.roll(from_high[at], (4 - 4 * k) % 128, 1)
            if emission:
                left = pltpu.roll(from_low[at], (9 - 4 * k) % 128, 1)
                value = strips[f, v] + jnp.where(is_right, right, 0.0) + jnp.where(is_left_e, left, 0.0)
            else:
                left = pltpu.roll(from_low[at], (8 - 4 * k) % 128, 1)
                value = jnp.where(is_right, right, jnp.where(is_left, left, strips[f, v]))
            joined[f, v] = value
            done[f, v] = value
    half = width // 2
    for p in range(fields // 2):
        a, b = 2 * p, 2 * p + 1
        high = jnp.where(lane >= half, done[a, owned - 1], pltpu.roll(done[b, owned - 1], half, 1))
        low = jnp.where(lane < half, done[a, 0], pltpu.roll(done[b, 0], half, 1))
        to0[p] = jnp.where(even, high, low)
        to1[p] = jnp.where(even, low, high)
    tail = jnp.zeros((8, 128), jnp.float32)
    for g in range(groups):
        moved = pltpu.roll(done[fields - groups + g, owned], 16 * g, 1) if g else done[fields - groups, owned]
        tail = jnp.where((lane >= 16 * g) & (lane < 16 * g + 16), moved, tail)
    to0[fields // 2] = tail
    to1[fields // 2] = tail


def closure(state):
    photons, flux = state[0], state[1:]
    inverse = 1.0 / photons
    unit = [f * inverse for f in flux]
    fsq = jnp.minimum(unit[0] * unit[0] + unit[1] * unit[1] + unit[2] * unit[2], 1.0)
    square = 4.0 - 3.0 * fsq
    root = square * lax.rsqrt(square)
    shape_term = 3.0 / (2.0 + root)
    diag = (root - 1.0) * (photons * (1.0 / 3.0))
    scaled = [f * shape_term for f in flux]
    xx, yy, zz = (scaled[a] * unit[a] + diag for a in range(3))
    xy, xz, yz = scaled[0] * unit[1], scaled[0] * unit[2], scaled[1] * unit[2]
    return ((flux[0], xx, xy, xz), (flux[1], xy, yy, yz), (flux[2], xz, yz, zz))


def chemistry(state, ion, dens):
    groups = len(state)
    reach = DT * dens
    loss = ALPHA * reach
    push = [state[g][0] * (DT * SIGMA[g]) for g in range(groups)]
    frac = ion
    for step in range(CHEM_ITERS):
        free = reach * (1.0 - frac)
        atten = [1.0 / (1.0 + SIGMA[g] * free) for g in range(groups)]
        gamma = sum((push[g] * atten[g] for g in range(1, groups)), push[0] * atten[0])
        frac = (ion + gamma) / (1.0 + (gamma + loss * frac))
    return [[u * atten[g] for u in state[g]] for g in range(groups)], frac


def strip_step(s_ref, t_ref, tiles, groups, comps, depth, update):
    fields = groups * comps
    keep, share = 1.0 - 3.0 * DT, 0.5 * DT
    lane = strip_lane()
    column = lax.rem(lane, 16)
    states = [
        [[s_ref[g * comps + c, v] for c in range(comps)] for g in range(groups)] for v in range(tiles)
    ]
    phys = [[closure(states[v][g]) for g in range(groups)] for v in range(tiles)]
    for v in range(tiles):
        for g in range(groups):
            for c in range(comps):
                u, f = states[v][g][c], phys[v][g][1][c]
                t_ref[g * comps + c, v] = jnp.where(column == 11, u + f, pltpu.roll(u - f, 6, 1))
    if not update:
        return
    for v in range(tiles):
        new = []
        for g in range(groups):
            comp = []
            for c in range(comps):
                u = states[v][g][c]
                fx, fy, fz = (phys[v][g][a][c] for a in range(3))
                vn, vp = (v + 1) % tiles, (v - 1) % tiles
                down, here_d = states[vn][g][c] - phys[vn][g][0][c], u - fx
                up, here_u = states[vp][g][c] + phys[vp][g][0][c], u + fx
                total = pltpu.roll(jnp.where(lane < 16, down, here_d), 112, 1)
                total = total + pltpu.roll(jnp.where(lane >= 112, up, here_u), 16, 1)
                total = total + pltpu.roll(u - fy, 127, 1) + pltpu.roll(u + fy, 1, 1)
                total = total + pltpu.roll(u - fz, depth - 1, 0) + pltpu.roll(u + fz, 1, 0)
                comp.append(keep * u + share * total)
            comp[0] = comp[0] + s_ref[fields + 2 + g, v]
            new.append(comp)
        new, frac = chemistry(new, s_ref[fields, v], s_ref[fields + 1, v])
        for g in range(groups):
            for c in range(comps):
                s_ref[g * comps + c, v] = new[g][c]
        s_ref[fields, v] = frac


def sweep(lo, hi, read, source, ion_of, den_of, write, t_ref, groups, comps, first_up=None, last_down=None):
    keep, share = 1.0 - 3.0 * DT, 0.5 * DT
    lane = strip_lane()
    depth, width = lane.shape
    cycle = 8 * t_ref.shape[1]

    def row_terms(x, inside):
        row = x % cycle
        v, group = row // 8, row % 8
        up, down, rest = [], [], []
        for g in range(groups):
            state = [read(g * comps + c, x) for c in range(comps)]
            px, py, pz = closure(state)
            for c in range(comps):
                u = state[c]
                up.append(u + px[c])
                down.append(u - px[c])
                if inside:
                    edge = pltpu.roll(t_ref[g * comps + c, v], (117 - 16 * group) % 128, 1)
                    total = jnp.where(lane == width - 1, edge, pltpu.roll(u - py[c], width - 1, 1))
                    total = total + jnp.where(lane == 0, edge, pltpu.roll(u + py[c], 1, 1))
                    total = total + pltpu.roll(u - pz[c], depth - 1, 0)
                    total = total + pltpu.roll(u + pz[c], 1, 0)
                    rest.append(keep * u + share * total)
        return up, down, rest

    before = row_terms(lo - 1, False)[0] if first_up is None else first_up
    here, low_down, rest = row_terms(lo, True)
    for x in range(lo, hi):
        if x + 1 < hi:
            after, down, rest_after = row_terms(x + 1, True)
        else:
            after, rest_after = None, None
            down = row_terms(hi, False)[1] if last_down is None else last_down
        new = []
        for g in range(groups):
            comp = []
            for c in range(comps):
                k = g * comps + c
                comp.append(rest[k] + share * (before[k] + down[k]))
            comp[0] = comp[0] + source(g, x)
            new.append(comp)
        new, frac = chemistry(new, ion_of(x), den_of(x))
        write(x, [new[g][c] for g in range(groups) for c in range(comps)], frac)
        if x + 1 < hi:
            before, here, rest = here, after, rest_after
    return low_down, here


def inner_kernel(rad, ion, den, joined, emis, u_ref, ion_ref, saved, s_ref, e_ref, t_ref):
    groups, comps, depth, rows_x, width = sizes_of(emis, rad.shape[0])
    tiles = rows_x // 8
    fields = groups * comps
    lane = strip_lane()
    for g in range(groups):
        for c in range(comps):
            for x in range(rows_x):
                u_ref[g * comps + c, x] = rad[g * comps + c, pl.ds(x, depth, stride=rows_x), :]
    for x in range(rows_x):
        ion_ref[x] = ion[pl.ds(x, depth, stride=rows_x), :]
    for f in range(fields + 2):
        for v in range(tiles):
            s_ref[f, v] = joined[f, v]
    for g in range(groups):
        f = fields + 2 + g
        for v in range(tiles):
            s_ref[f, v] = joined[f, v] * DT
        for x in range(1, rows_x - 1):
            v, group = x // 8, x % 8
            edge = pltpu.roll(s_ref[f, v], (116 - 16 * group) % 128, 1)
            e_ref[g, x] = jnp.where(lane == 0, edge, emis[g, x] * DT)

    def write(x, values, frac):
        for k, value in enumerate(values):
            u_ref[k, x] = value
        ion_ref[x] = frac

    for step in range(SUBSTEPS):
        strip_step(s_ref, t_ref, tiles, groups, comps, depth, step < SUBSTEPS - 1)
        down, up = sweep(
            step + 1,
            rows_x - 1 - step,
            lambda k, x: u_ref[k, x],
            lambda g, x: e_ref[g, x],
            lambda x: ion_ref[x],
            lambda x: den[pl.ds(x, depth, stride=rows_x), :],
            write,
            t_ref,
            groups,
            comps,
        )
        for k in range(fields):
            saved[0, step, k] = down[k]
            saved[1, step, k] = up[k]


def outer_kernel(
    u_mid, ion_mid, saved, den, from0, from1, joined, corner0, corner1, emis,
    rad_out, ion_out, u_ref, ion_ref, s_ref, e_ref, t_ref,
):
    even = lax.rem(lax.axis_index("gx"), 2) == 0
    groups, comps, depth, rows_x, width = sizes_of(emis, rad_out.shape[0])
    tiles = joined.shape[1]
    owned = tiles - 1
    cycle = 8 * tiles
    fields = groups * comps
    inner_at, emis_at, _ = halo_parts(fields, 2, groups)
    lane = strip_lane()

    def beside(at, first=from0, second=from1):
        a, b = first[at], second[at]
        return jnp.where(even, b, a), jnp.where(even, a, b)

    half = width // 2
    strip_fields = fields + 2 + groups
    for p in range(strip_fields // 2):
        below, above = beside(p, corner0, corner1)
        s_ref[2 * p, owned] = jnp.where(lane < half, above, below)
        s_ref[2 * p + 1, owned] = pltpu.roll(jnp.where(lane < half, below, above), half, 1)
        for f in (2 * p, 2 * p + 1):
            for v in range(owned):
                s_ref[f, v] = joined[f, v]
    edge_rows = list(range(-INNER, HALO)) + list(range(rows_x - HALO, rows_x + INNER))
    tail, _ = beside(strip_fields // 2, corner0, corner1)
    for g in range(groups):
        f = fields + 2 + g
        row_16 = pltpu.roll(tail, (-16 * g) % 128, 1) if g else tail
        s_ref[f, 0] = (s_ref[f, 0] + jnp.where(lane < 16, row_16, 0.0)) * DT
        for v in range(1, owned):
            s_ref[f, v] = s_ref[f, v] * DT
        s_ref[f, owned] = (s_ref[f, owned] + joined[f, owned]) * DT
        for x in edge_rows:
            parts = []
            if 0 <= x <= rows_x:
                parts.append(emis[g, x])
            if x <= 0:
                parts.append(beside(emis_at + g * (INNER + 1) + x + INNER)[0])
            if x >= rows_x:
                parts.append(beside(emis_at + g * (INNER + 1) + x - rows_x)[1])
            total = sum(parts[1:], parts[0])
            row = x % cycle
            v, group = row // 8, row % 8
            edge = pltpu.roll(s_ref[f, v], (116 - 16 * group) % 128, 1)
            e_ref[g, x + HALO] = jnp.where(lane == 0, edge, total * DT)

    for f in range(fields):
        for i in range(HALO):
            below, above = beside(f * HALO + i)
            u_ref[f, i] = below
            u_ref[f, rows_x + HALO + i] = above
            u_ref[f, HALO + i] = u_mid[f, i]
            u_ref[f, rows_x + i] = u_mid[f, rows_x - HALO + i]
    for i in range(HALO):
        ion_ref[HALO + i] = ion_mid[i]
        ion_ref[rows_x + i] = ion_mid[rows_x - HALO + i]
    for i in range(INNER):
        below, above = beside(inner_at + i)
        ion_ref[i + 1] = below
        ion_ref[rows_x + HALO + i] = above

    def den_of(x):
        if x < 0:
            return beside(inner_at + INNER + x + INNER)[0]
        if x >= rows_x:
            return beside(inner_at + INNER + x - rows_x)[1]
        return den[pl.ds(x, depth, stride=rows_x), :]

    def finish(x, values, frac):
        for k, value in enumerate(values):
            rad_out[k, pl.ds(x, depth, stride=rows_x), :] = value
        ion_out[pl.ds(x, depth, stride=rows_x), :] = frac

    def write(x, values, frac):
        for k, value in enumerate(values):
            u_ref[k, x + HALO] = value
        ion_ref[x + HALO] = frac

    for x in range(HALO, rows_x - HALO):
        finish(x, [u_mid[k, x] for k in range(fields)], ion_mid[x])

    for step in range(SUBSTEPS):
        strip_step(s_ref, t_ref, tiles, groups, comps, depth, step < SUBSTEPS - 1)
        last = step == SUBSTEPS - 1
        common = (
            lambda k, x: u_ref[k, x + HALO],
            lambda g, x: e_ref[g, x + HALO],
            lambda x: ion_ref[x + HALO],
            den_of,
            finish if last else write,
            t_ref,
            groups,
            comps,
        )
        rest = INNER - step
        sweep(-rest, step + 1, *common, last_down=[saved[0, step, k] for k in range(fields)])
        sweep(
            rows_x - 1 - step,
            rows_x + rest,
            *common,
            first_up=[saved[1, step, k] for k in range(fields)],
        )


def on_device(radiation, ion_fraction, density, star_lum, star_cell, star_offset, star_count):
    groups, comps, depth, rows_x, width = radiation.shape
    slots = star_lum.shape[3]
    fields = groups * comps
    strip_fields = fields + 2 + groups
    nx, ny = lax.axis_size("gx"), lax.axis_size("gy")
    if depth != 8 or width != 128 or rows_x % 8 or groups != len(SIGMA) or strip_fields % 4 or rows_x < 2 * HALO:
        raise ValueError("tile shape")
    if nx % 2:
        raise ValueError("odd axis")
    owned = rows_x // 8
    tiles = owned + 1
    f32 = jnp.float32
    plane = (depth, width)
    rows = rows_x + 2 * HALO
    planes = halo_parts(fields, 2, groups)[2]
    vmem = pl.BlockSpec(memory_space=pltpu.VMEM)
    hbm = pl.BlockSpec(memory_space=pltpu.HBM)
    small = pltpu.CompilerParams(vmem_limit_bytes=8 * 1024 * 1024)

    def out(*shape):
        return jax.ShapeDtypeStruct(shape + plane, f32)

    shapes = radiation.shape, ion_fraction.shape
    radiation = radiation.reshape(fields, depth * rows_x, width)
    ion_fraction = ion_fraction.reshape(depth * rows_x, width)
    density = density.reshape(depth * rows_x, width)
    star_cell = star_cell.reshape(3, 1, slots)
    star_offset = star_offset.reshape(3, 1, slots)
    arrays = (radiation, ion_fraction, density, star_lum, star_cell, star_offset, star_count)
    sent = strip_fields // 4 * owned + 1
    low_y, high_y, to0, to1, strips, emis = pl.pallas_call(
        pack_kernel,
        out_shape=[
            out(sent), out(sent), out(planes), out(planes), out(strip_fields, tiles), out(groups, rows_x + 1)
        ],
        in_specs=[hbm] * 7,
        scratch_shapes=[pltpu.VMEM(a.shape, a.dtype) for a in arrays] + [pltpu.SemaphoreType.DMA((7,))],
        compiler_params=small,
        name="pack",
    )(*[pltpu.with_memory_space_constraint(a, pltpu.HBM) for a in arrays[:6]], star_count)
    up = [(i, (i + 1) % ny) for i in range(ny)]
    down = [((i + 1) % ny, i) for i in range(ny)]
    from_low = lax.ppermute(high_y, "gy", up)
    from_high = lax.ppermute(low_y, "gy", down)
    from0 = lax.ppermute(to0, "gx", neighbour_pairs(nx, 0))
    from1 = lax.ppermute(to1, "gx", neighbour_pairs(nx, 1))
    joined, edge0, edge1 = pl.pallas_call(
        edge_kernel,
        out_shape=[out(strip_fields, tiles), out(strip_fields // 2 + 1), out(strip_fields // 2 + 1)],
        in_specs=[vmem] * 3,
        compiler_params=small,
        name="edges",
    )(strips, from_low, from_high)
    corner0 = lax.ppermute(edge0, "gx", neighbour_pairs(nx, 0))
    corner1 = lax.ppermute(edge1, "gx", neighbour_pairs(nx, 1))
    u_mid, ion_mid, saved = pl.pallas_call(
        inner_kernel,
        out_shape=[out(fields, rows_x), out(rows_x), out(2, SUBSTEPS, fields)],
        in_specs=[vmem] * 5,
        scratch_shapes=[
            pltpu.VMEM((strip_fields, owned) + plane, f32),
            pltpu.VMEM((groups, rows_x) + plane, f32),
            pltpu.VMEM((fields, owned) + plane, f32),
        ],
        compiler_params=small,
        cost_estimate=pl.CostEstimate(flops=40_000_000, bytes_accessed=2_000_000, transcendentals=0),
        name="inner_rows",
    )(radiation, ion_fraction, density, joined, emis)
    return tuple(
        result.reshape(shape)
        for shape, result in zip(shapes, pl.pallas_call(
            outer_kernel,
            out_shape=[
                jax.ShapeDtypeStruct(radiation.shape, f32),
                jax.ShapeDtypeStruct(ion_fraction.shape, f32),
            ],
            in_specs=[vmem] * 10,
            scratch_shapes=[
                pltpu.VMEM((fields, rows) + plane, f32),
                pltpu.VMEM((rows,) + plane, f32),
                pltpu.VMEM((strip_fields, tiles) + plane, f32),
                pltpu.VMEM((groups, rows) + plane, f32),
                pltpu.VMEM((fields, tiles) + plane, f32),
            ],
            compiler_params=small,
            name="outer_rows",
        )(u_mid, ion_mid, saved, density, from0, from1, joined, corner0, corner1, emis))
    )


def solution(mesh):
    return jax.shard_map(
        on_device,
        mesh=mesh,
        in_specs=(
            P(None, None, None, "gx", "gy"),
            P(None, "gx", "gy"),
            P(None, "gx", "gy"),
            P("gx", "gy", None, None),
            P("gx", "gy", None, None),
            P("gx", "gy", None, None),
            P("gx", "gy"),
        ),
        out_specs=(P(None, None, None, "gx", "gy"), P(None, "gx", "gy")),
        check_vma=False,
    )
```

```python
import jax
import jax.numpy as jnp
from jax import lax
from jax.experimental import pallas as pl
from jax.experimental.pallas import tpu as pltpu
from jax.sharding import PartitionSpec as P


SUBSTEPS = 4
CHEM_ITERS = 3
DT = 0.3
ALPHA = 0.4
SIGMA = (1.5, 0.5)

HALO = SUBSTEPS
INNER = HALO - 1


def neighbour_pairs(count, parity):
    return [(i, (i + 1) % count if i % 2 == parity else (i - 1) % count) for i in range(count)]


def halo_parts(fields_full, fields_inner, groups):
    inner = fields_full * HALO
    emis = inner + fields_inner * INNER
    return inner, emis, emis + groups * (INNER + 1)


def deposit(stars, rows, depth, width):
    lum, cell, off = stars
    slots = lum[0].shape[1]
    z = lax.broadcasted_iota(jnp.int32, (depth, slots), 0)
    upper = jnp.where(cell[2] + 1 == depth, 0, cell[2] + 1)
    weight_z = jnp.where(z == cell[2], 1.0 - off[2], 0.0) + jnp.where(z == upper, off[2], 0.0)
    y = lax.broadcasted_iota(jnp.int32, (2 * width, slots), 0)
    weight_y = jnp.where(y == cell[1], 1.0 - off[1], 0.0) + jnp.where(y == cell[1] + 1, off[1], 0.0)
    left = []
    for light in lum:
        for x in rows:
            weight_x = jnp.where(cell[0] == x, 1.0 - off[0], 0.0)
            weight_x = weight_x + jnp.where(cell[0] == x - 1, off[0], 0.0)
            left.append(weight_z * (weight_x * light))
    return lax.dot_general(
        jnp.concatenate(left, axis=0),
        weight_y,
        (((1,), (1,)), ((), ())),
        precision=lax.Precision.HIGHEST,
        preferred_element_type=jnp.float32,
    )


def sizes_of(emis, fields):
    groups, rows, depth, width = emis.shape
    return groups, fields // groups, depth, rows - 1, width


def strip_lane():
    return lax.broadcasted_iota(jnp.int32, (8, 128), 1)


def pack_kernel(
    rad_hbm, ion_hbm, den_hbm, lum_hbm, cell_hbm, off_hbm, count_hbm,
    low_y, high_y, to0, to1, strips, emis,
    rad, ion, den, lum_ref, cell_ref, off_ref, count_ref, sem,
):
    even = lax.rem(lax.axis_index("gx"), 2) == 0
    copies = [
        pltpu.make_async_copy(src, dst, sem.at[k])
        for k, (src, dst) in enumerate(
            (
                (lum_hbm, lum_ref),
                (cell_hbm, cell_ref),
                (off_hbm, off_ref),
                (count_hbm, count_ref),
                (rad_hbm, rad),
                (ion_hbm, ion),
                (den_hbm, den),
            )
        )
    ]
    for copy in copies:
        copy.start()
    groups, comps, depth, rows_x, width = sizes_of(emis, rad.shape[0])
    owned = rows_x // 8
    lane = strip_lane()
    column = lax.rem(lane, 16)
    zero = jnp.zeros((8, 128), jnp.float32)
    for copy in copies[:4]:
        copy.wait()
    slots = lum_ref.shape[3]
    slot = lax.broadcasted_iota(jnp.int32, (1, slots), 1)
    live = (slot < count_ref[...]).astype(jnp.float32)
    stars = (
        [lum_ref[0, 0, g : g + 1, :] * live for g in range(groups)],
        [cell_ref[a] for a in range(3)],
        [off_ref[a] for a in range(3)],
    )
    table = deposit(stars, range(rows_x + 1), depth, width)

    def plane_of(g, x, half):
        start = (g * (rows_x + 1) + x) * depth
        return table[start : start + depth, half * width : (half + 1) * width]

    for copy in copies[4:]:
        copy.wait()
    reads = [(lambda x, f=f: rad[f, pl.ds(x, depth, stride=rows_x), :]) for f in range(groups * comps)]
    reads += [lambda x: ion[pl.ds(x, depth, stride=rows_x), :], lambda x: den[pl.ds(x, depth, stride=rows_x), :]]
    fields = len(reads)
    packs_low = [[zero] * owned for _ in range((fields + groups) // 4)]
    packs_high = [[zero] * owned for _ in range((fields + groups) // 4)]
    tail_low, tail_high = zero, zero

    def add(pack, k, part, source):
        return jnp.where((column >= 4 * k) & (column < 4 * k + 4), pltpu.roll(part, (4 * k - source) % 128, 1), pack)

    for f, read in enumerate(reads):
        for v in range(owned):
            acc = zero
            for group in range(8):
                low = pltpu.roll(read(8 * v + group), (16 * group + 4) % 128, 1)
                at = lane - 16 * group
                acc = jnp.where((at >= 0) & (at < 8), low, acc)
            acc = jnp.where(column < 8, acc, pltpu.roll(acc, 8, 1))
            strips[f, v] = acc
            p, k = f // 4, f % 4
            packs_high[p][v] = add(packs_high[p][v], k, acc, 8)
            packs_low[p][v] = add(packs_low[p][v], k, acc, 4)
    for g in range(groups):
        f = fields + g
        p, k = f // 4, f % 4
        near, past = [zero] * (owned + 1), [zero] * (owned + 1)
        for x in range(rows_x + 1):
            v, group = x // 8, x % 8
            plane = plane_of(g, x, 0)
            emis[g, x] = plane
            at = lane - 16 * group
            low = pltpu.roll(plane, (16 * group + 4) % 128, 1)
            near[v] = jnp.where((at >= 0) & (at < 8), low, near[v])
            over = plane_of(g, x, 1)
            over = pltpu.roll(over, 16 * group, 1) if group else over
            past[v] = jnp.where(at == 0, over, past[v])
        sent, own = [], []
        for v in range(owned + 1):
            far = pltpu.roll(near[v], 8, 1)
            s = jnp.where((column >= 4) & (column < 8), near[v], 0.0)
            s = jnp.where((column >= 8) & (column < 12), far, s)
            sent.append(jnp.where(column == 12, pltpu.roll(past[v], 12, 1), s))
            o = jnp.where(column < 4, near[v], jnp.where(column >= 12, far, 0.0))
            own.append(jnp.where(column == 4, pltpu.roll(past[v], 4, 1), o))
        for v in range(owned + 1):
            strips[f, v] = own[v]
        for v in range(owned):
            packs_high[p][v] = add(packs_high[p][v], k, sent[v], 9)
            packs_low[p][v] = add(packs_low[p][v], k, sent[v], 4)
        tail_high = add(tail_high, k, sent[owned], 9)
        tail_low = add(tail_low, k, sent[owned], 4)
    for p in range(len(packs_low)):
        for v in range(owned):
            high_y[p * owned + v] = packs_high[p][v]
            low_y[p * owned + v] = packs_low[p][v]
    high_y[len(packs_low) * owned] = tail_high
    low_y[len(packs_low) * owned] = tail_low

    at = 0

    def put(high, low):
        nonlocal at
        to0[at] = jnp.where(even, high, low)
        to1[at] = jnp.where(even, low, high)
        at += 1

    for read in reads[: groups * comps]:
        for i in range(HALO):
            put(read(rows_x - HALO + i), read(i))
    for read in reads[groups * comps :]:
        for i in range(INNER):
            put(read(rows_x - INNER + i), read(i))
    for g in range(groups):
        for i in range(INNER + 1):
            put(plane_of(g, rows_x - INNER + i, 0), plane_of(g, i, 0))


def edge_kernel(strips, from_low, from_high, joined, to0, to1):
    even = lax.rem(lax.axis_index("gx"), 2) == 0
    fields, tiles, _, width = strips.shape
    owned = tiles - 1
    groups = len(SIGMA)
    lane = strip_lane()
    column = lax.rem(lane, 16)
    is_right = (column >= 4) & (column < 8)
    is_left = (column >= 8) & (column < 12)
    is_left_e = (column >= 9) & (column < 13)
    done = {}
    for f in range(fields):
        emission = f >= fields - groups
        p, k = f // 4, f % 4
        for v in range(tiles if emission else owned):
            at = p * owned + v
            right = pltpu.roll(from_high[at], (4 - 4 * k) % 128, 1)
            if emission:
                left = pltpu.roll(from_low[at], (9 - 4 * k) % 128, 1)
                value = strips[f, v] + jnp.where(is_right, right, 0.0) + jnp.where(is_left_e, left, 0.0)
            else:
                left = pltpu.roll(from_low[at], (8 - 4 * k) % 128, 1)
                value = jnp.where(is_right, right, jnp.where(is_left, left, strips[f, v]))
            joined[f, v] = value
            done[f, v] = value
    half = width // 2
    for p in range(fields // 2):
        a, b = 2 * p, 2 * p + 1
        high = jnp.where(lane >= half, done[a, owned - 1], pltpu.roll(done[b, owned - 1], half, 1))
        low = jnp.where(lane < half, done[a, 0], pltpu.roll(done[b, 0], half, 1))
        to0[p] = jnp.where(even, high, low)
        to1[p] = jnp.where(even, low, high)
    tail = jnp.zeros((8, 128), jnp.float32)
    for g in range(groups):
        moved = pltpu.roll(done[fields - groups + g, owned], 16 * g, 1) if g else done[fields - groups, owned]
        tail = jnp.where((lane >= 16 * g) & (lane < 16 * g + 16), moved, tail)
    to0[fields // 2] = tail
    to1[fields // 2] = tail


def closure(state):
    photons, flux = state[0], state[1:]
    inverse = 1.0 / photons
    unit = [f * inverse for f in flux]
    fsq = jnp.minimum(unit[0] * unit[0] + unit[1] * unit[1] + unit[2] * unit[2], 1.0)
    square = 4.0 - 3.0 * fsq
    root = square * lax.rsqrt(square)
    shape_term = 3.0 / (2.0 + root)
    diag = (root - 1.0) * (photons * (1.0 / 3.0))
    scaled = [f * shape_term for f in flux]
    xx, yy, zz = (scaled[a] * unit[a] + diag for a in range(3))
    xy, xz, yz = scaled[0] * unit[1], scaled[0] * unit[2], scaled[1] * unit[2]
    return ((flux[0], xx, xy, xz), (flux[1], xy, yy, yz), (flux[2], xz, yz, zz))


def chemistry(state, ion, dens):
    groups = len(state)
    reach = DT * dens
    loss = ALPHA * reach
    push = [state[g][0] * (DT * SIGMA[g]) for g in range(groups)]
    frac = ion
    for _ in range(CHEM_ITERS):
        free = reach * (1.0 - frac)
        atten = [1.0 / (1.0 + SIGMA[g] * free) for g in range(groups)]
        gamma = sum((push[g] * atten[g] for g in range(1, groups)), push[0] * atten[0])
        frac = (ion + gamma) / (1.0 + (gamma + loss * frac))
    return [[u * atten[g] for u in state[g]] for g in range(groups)], frac


def strip_step(s_ref, t_ref, tiles, groups, comps, depth, update):
    fields = groups * comps
    keep, share = 1.0 - 3.0 * DT, 0.5 * DT
    lane = strip_lane()
    column = lax.rem(lane, 16)
    states = [
        [[s_ref[g * comps + c, v] for c in range(comps)] for g in range(groups)] for v in range(tiles)
    ]
    phys = [[closure(states[v][g]) for g in range(groups)] for v in range(tiles)]
    for v in range(tiles):
        for g in range(groups):
            for c in range(comps):
                u, f = states[v][g][c], phys[v][g][1][c]
                t_ref[g * comps + c, v] = jnp.where(column == 11, u + f, pltpu.roll(u - f, 6, 1))
    if not update:
        return
    for v in range(tiles):
        new = []
        for g in range(groups):
            comp = []
            for c in range(comps):
                u = states[v][g][c]
                fx, fy, fz = (phys[v][g][a][c] for a in range(3))
                vn, vp = (v + 1) % tiles, (v - 1) % tiles
                down, here_d = states[vn][g][c] - phys[vn][g][0][c], u - fx
                up, here_u = states[vp][g][c] + phys[vp][g][0][c], u + fx
                total = pltpu.roll(jnp.where(lane < 16, down, here_d), 112, 1)
                total = total + pltpu.roll(jnp.where(lane >= 112, up, here_u), 16, 1)
                total = total + pltpu.roll(u - fy, 127, 1) + pltpu.roll(u + fy, 1, 1)
                total = total + pltpu.roll(u - fz, depth - 1, 0) + pltpu.roll(u + fz, 1, 0)
                comp.append(keep * u + share * total)
            comp[0] = comp[0] + s_ref[fields + 2 + g, v]
            new.append(comp)
        new, frac = chemistry(new, s_ref[fields, v], s_ref[fields + 1, v])
        for g in range(groups):
            for c in range(comps):
                s_ref[g * comps + c, v] = new[g][c]
        s_ref[fields, v] = frac


def sweep(lo, hi, read, source, ion_of, den_of, write, t_ref, groups, comps, first_up=None, last_down=None):
    keep, share = 1.0 - 3.0 * DT, 0.5 * DT
    lane = strip_lane()
    depth, width = lane.shape
    cycle = 8 * t_ref.shape[1]

    def row_terms(x, inside):
        row = x % cycle
        v, group = row // 8, row % 8
        up, down, rest = [], [], []
        for g in range(groups):
            state = [read(g * comps + c, x) for c in range(comps)]
            px, py, pz = closure(state)
            for c in range(comps):
                u = state[c]
                up.append(u + px[c])
                down.append(u - px[c])
                if inside:
                    edge = pltpu.roll(t_ref[g * comps + c, v], (117 - 16 * group) % 128, 1)
                    total = jnp.where(lane == width - 1, edge, pltpu.roll(u - py[c], width - 1, 1))
                    total = total + jnp.where(lane == 0, edge, pltpu.roll(u + py[c], 1, 1))
                    total = total + pltpu.roll(u - pz[c], depth - 1, 0)
                    total = total + pltpu.roll(u + pz[c], 1, 0)
                    rest.append(keep * u + share * total)
        return up, down, rest

    before = row_terms(lo - 1, False)[0] if first_up is None else first_up
    here, low_down, rest = row_terms(lo, True)
    for x in range(lo, hi):
        if x + 1 < hi:
            after, down, rest_after = row_terms(x + 1, True)
        else:
            after, rest_after = None, None
            down = row_terms(hi, False)[1] if last_down is None else last_down
        new = []
        for g in range(groups):
            comp = []
            for c in range(comps):
                k = g * comps + c
                comp.append(rest[k] + share * (before[k] + down[k]))
            comp[0] = comp[0] + source(g, x)
            new.append(comp)
        new, frac = chemistry(new, ion_of(x), den_of(x))
        write(x, [new[g][c] for g in range(groups) for c in range(comps)], frac)
        if x + 1 < hi:
            before, here, rest = here, after, rest_after
    return low_down, here


def inner_kernel(rad, ion, den, joined, emis, u_ref, ion_ref, saved, s_ref, e_ref, t_ref):
    groups, comps, depth, rows_x, _ = sizes_of(emis, rad.shape[0])
    tiles = rows_x // 8
    fields = groups * comps
    lane = strip_lane()
    for g in range(groups):
        for c in range(comps):
            for x in range(rows_x):
                u_ref[g * comps + c, x] = rad[g * comps + c, pl.ds(x, depth, stride=rows_x), :]
    for x in range(rows_x):
        ion_ref[x] = ion[pl.ds(x, depth, stride=rows_x), :]
    for f in range(fields + 2):
        for v in range(tiles):
            s_ref[f, v] = joined[f, v]
    for g in range(groups):
        f = fields + 2 + g
        for v in range(tiles):
            s_ref[f, v] = joined[f, v] * DT
        for x in range(1, rows_x - 1):
            v, group = x // 8, x % 8
            edge = pltpu.roll(s_ref[f, v], (116 - 16 * group) % 128, 1)
            e_ref[g, x] = jnp.where(lane == 0, edge, emis[g, x] * DT)

    def write(x, values, frac):
        for k, value in enumerate(values):
            u_ref[k, x] = value
        ion_ref[x] = frac

    for step in range(SUBSTEPS):
        strip_step(s_ref, t_ref, tiles, groups, comps, depth, step < SUBSTEPS - 1)
        down, up = sweep(
            step + 1,
            rows_x - 1 - step,
            lambda k, x: u_ref[k, x],
            lambda g, x: e_ref[g, x],
            lambda x: ion_ref[x],
            lambda x: den[pl.ds(x, depth, stride=rows_x), :],
            write,
            t_ref,
            groups,
            comps,
        )
        for k in range(fields):
            saved[0, step, k] = down[k]
            saved[1, step, k] = up[k]


def outer_kernel(
    u_mid, ion_mid, saved, den, from0, from1, joined, corner0, corner1, emis,
    rad_out, ion_out, u_ref, ion_ref, s_ref, e_ref, t_ref,
):
    even = lax.rem(lax.axis_index("gx"), 2) == 0
    groups, comps, depth, rows_x, width = sizes_of(emis, rad_out.shape[0])
    tiles = joined.shape[1]
    owned = tiles - 1
    cycle = 8 * tiles
    fields = groups * comps
    inner_at, emis_at, _ = halo_parts(fields, 2, groups)
    lane = strip_lane()

    def beside(at, first=from0, second=from1):
        a, b = first[at], second[at]
        return jnp.where(even, b, a), jnp.where(even, a, b)

    half = width // 2
    strip_fields = fields + 2 + groups
    for p in range(strip_fields // 2):
        below, above = beside(p, corner0, corner1)
        s_ref[2 * p, owned] = jnp.where(lane < half, above, below)
        s_ref[2 * p + 1, owned] = pltpu.roll(jnp.where(lane < half, below, above), half, 1)
        for f in (2 * p, 2 * p + 1):
            for v in range(owned):
                s_ref[f, v] = joined[f, v]
    edge_rows = list(range(-INNER, HALO)) + list(range(rows_x - HALO, rows_x + INNER))
    tail, _ = beside(strip_fields // 2, corner0, corner1)
    for g in range(groups):
        f = fields + 2 + g
        row_16 = pltpu.roll(tail, (-16 * g) % 128, 1) if g else tail
        s_ref[f, 0] = (s_ref[f, 0] + jnp.where(lane < 16, row_16, 0.0)) * DT
        for v in range(1, owned):
            s_ref[f, v] = s_ref[f, v] * DT
        s_ref[f, owned] = (s_ref[f, owned] + joined[f, owned]) * DT
        for x in edge_rows:
            parts = []
            if 0 <= x <= rows_x:
                parts.append(emis[g, x])
            if x <= 0:
                parts.append(beside(emis_at + g * (INNER + 1) + x + INNER)[0])
            if x >= rows_x:
                parts.append(beside(emis_at + g * (INNER + 1) + x - rows_x)[1])
            total = sum(parts[1:], parts[0])
            row = x % cycle
            v, group = row // 8, row % 8
            edge = pltpu.roll(s_ref[f, v], (116 - 16 * group) % 128, 1)
            e_ref[g, x + HALO] = jnp.where(lane == 0, edge, total * DT)

    for f in range(fields):
        for i in range(HALO):
            below, above = beside(f * HALO + i)
            u_ref[f, i] = below
            u_ref[f, rows_x + HALO + i] = above
            u_ref[f, HALO + i] = u_mid[f, i]
            u_ref[f, rows_x + i] = u_mid[f, rows_x - HALO + i]
    for i in range(HALO):
        ion_ref[HALO + i] = ion_mid[i]
        ion_ref[rows_x + i] = ion_mid[rows_x - HALO + i]
    for i in range(INNER):
        below, above = beside(inner_at + i)
        ion_ref[i + 1] = below
        ion_ref[rows_x + HALO + i] = above

    def den_of(x):
        if x < 0:
            return beside(inner_at + INNER + x + INNER)[0]
        if x >= rows_x:
            return beside(inner_at + INNER + x - rows_x)[1]
        return den[pl.ds(x, depth, stride=rows_x), :]

    def finish(x, values, frac):
        for k, value in enumerate(values):
            rad_out[k, pl.ds(x, depth, stride=rows_x), :] = value
        ion_out[pl.ds(x, depth, stride=rows_x), :] = frac

    def write(x, values, frac):
        for k, value in enumerate(values):
            u_ref[k, x + HALO] = value
        ion_ref[x + HALO] = frac

    for x in range(HALO, rows_x - HALO):
        finish(x, [u_mid[k, x] for k in range(fields)], ion_mid[x])

    for step in range(SUBSTEPS):
        strip_step(s_ref, t_ref, tiles, groups, comps, depth, step < SUBSTEPS - 1)
        last = step == SUBSTEPS - 1
        common = (
            lambda k, x: u_ref[k, x + HALO],
            lambda g, x: e_ref[g, x + HALO],
            lambda x: ion_ref[x + HALO],
            den_of,
            finish if last else write,
            t_ref,
            groups,
            comps,
        )
        rest = INNER - step
        sweep(-rest, step + 1, *common, last_down=[saved[0, step, k] for k in range(fields)])
        sweep(
            rows_x - 1 - step,
            rows_x + rest,
            *common,
            first_up=[saved[1, step, k] for k in range(fields)],
        )


def on_device(radiation, ion_fraction, density, star_lum, star_cell, star_offset, star_count):
    groups, comps, depth, rows_x, width = radiation.shape
    slots = star_lum.shape[3]
    fields = groups * comps
    strip_fields = fields + 2 + groups
    nx, ny = lax.axis_size("gx"), lax.axis_size("gy")
    if depth != 8 or width != 128 or rows_x % 8 or groups != len(SIGMA) or strip_fields % 4 or rows_x < 2 * HALO:
        raise ValueError("tile shape")
    if nx % 2:
        raise ValueError("odd axis")
    owned = rows_x // 8
    tiles = owned + 1
    f32 = jnp.float32
    plane = (depth, width)
    rows = rows_x + 2 * HALO
    planes = halo_parts(fields, 2, groups)[2]
    vmem = pl.BlockSpec(memory_space=pltpu.VMEM)
    hbm = pl.BlockSpec(memory_space=pltpu.HBM)
    small = pltpu.CompilerParams(vmem_limit_bytes=8 * 1024 * 1024)

    def out(*shape):
        return jax.ShapeDtypeStruct(shape + plane, f32)

    shapes = radiation.shape, ion_fraction.shape
    radiation = radiation.reshape(fields, depth * rows_x, width)
    ion_fraction = ion_fraction.reshape(depth * rows_x, width)
    density = density.reshape(depth * rows_x, width)
    star_cell = star_cell.reshape(3, 1, slots)
    star_offset = star_offset.reshape(3, 1, slots)
    arrays = (radiation, ion_fraction, density, star_lum, star_cell, star_offset, star_count)
    sent = strip_fields // 4 * owned + 1
    low_y, high_y, to0, to1, strips, emis = pl.pallas_call(
        pack_kernel,
        out_shape=[
            out(sent), out(sent), out(planes), out(planes), out(strip_fields, tiles), out(groups, rows_x + 1)
        ],
        in_specs=[hbm] * 7,
        scratch_shapes=[pltpu.VMEM(a.shape, a.dtype) for a in arrays] + [pltpu.SemaphoreType.DMA((7,))],
        compiler_params=small,
        name="pack",
    )(*[pltpu.with_memory_space_constraint(a, pltpu.HBM) for a in arrays[:6]], star_count)
    up = [(i, (i + 1) % ny) for i in range(ny)]
    down = [((i + 1) % ny, i) for i in range(ny)]
    from1 = lax.ppermute(to1, "gx", neighbour_pairs(nx, 1))
    from_low = lax.ppermute(high_y, "gy", up)
    from_high = lax.ppermute(low_y, "gy", down)
    from0 = lax.ppermute(to0, "gx", neighbour_pairs(nx, 0))
    joined, edge0, edge1 = pl.pallas_call(
        edge_kernel,
        out_shape=[out(strip_fields, tiles), out(strip_fields // 2 + 1), out(strip_fields // 2 + 1)],
        in_specs=[vmem] * 3,
        compiler_params=small,
        name="edges",
    )(strips, from_low, from_high)
    corner0 = lax.ppermute(edge0, "gx", neighbour_pairs(nx, 0))
    corner1 = lax.ppermute(edge1, "gx", neighbour_pairs(nx, 1))
    u_mid, ion_mid, saved = pl.pallas_call(
        inner_kernel,
        out_shape=[out(fields, rows_x), out(rows_x), out(2, SUBSTEPS, fields)],
        in_specs=[vmem] * 5,
        scratch_shapes=[
            pltpu.VMEM((strip_fields, owned) + plane, f32),
            pltpu.VMEM((groups, rows_x) + plane, f32),
            pltpu.VMEM((fields, owned) + plane, f32),
        ],
        compiler_params=small,
        cost_estimate=pl.CostEstimate(flops=40_000_000, bytes_accessed=2_000_000, transcendentals=0),
        name="inner_rows",
    )(radiation, ion_fraction, density, joined, emis)
    return tuple(
        result.reshape(shape)
        for shape, result in zip(shapes, pl.pallas_call(
            outer_kernel,
            out_shape=[
                jax.ShapeDtypeStruct(radiation.shape, f32),
                jax.ShapeDtypeStruct(ion_fraction.shape, f32),
            ],
            in_specs=[vmem] * 10,
            scratch_shapes=[
                pltpu.VMEM((fields, rows) + plane, f32),
                pltpu.VMEM((rows,) + plane, f32),
                pltpu.VMEM((strip_fields, tiles) + plane, f32),
                pltpu.VMEM((groups, rows) + plane, f32),
                pltpu.VMEM((fields, tiles) + plane, f32),
            ],
            compiler_params=small,
            name="outer_rows",
        )(u_mid, ion_mid, saved, density, from0, from1, joined, corner0, corner1, emis))
    )


def solution(mesh):
    return jax.shard_map(
        on_device,
        mesh=mesh,
        in_specs=(
            P(None, None, None, "gx", "gy"),
            P(None, "gx", "gy"),
            P(None, "gx", "gy"),
            P("gx", "gy", None, None),
            P("gx", "gy", None, None),
            P("gx", "gy", None, None),
            P("gx", "gy"),
        ),
        out_specs=(P(None, None, None, "gx", "gy"), P(None, "gx", "gy")),
        check_vma=False,
    )
```
